32 devices in a mesh: row: 8 (over z, core), col: 4 (over y, x).
Axes of the slice: x: 2, y: 2, z: 4, core: 2. Of those that a mesh axis runs over, the one named last changes fastest.
Arguments:
- wrapped_phase: float32 [16384, 2048], P('row', 'col'), may hold values from -2.85 to 2.85, as said below
Outputs:
- unwrapped: float32 [16384, 2048], P('row', 'col')
The draws below stay inside these ranges and needn't reach their ends.
Inputs may be any that keep to these rules, and one draw needn't show every extreme that they name: The difference of wrapped_phase between any two adjacent cells of the map lies 0.14 or more away from every odd multiple of pi.
All inputs are finite; a program needn't handle non-finite values.
Results may differ from the reference program's by a relative error of at most 0.0003.
Values sent between devices are 32-bit elements; how exact they have to be, the bound alone decides.
A program may use at most 128 MiB of HBM per device.

```python
import math
import jax
import jax.numpy as jnp
from jax import lax

TILE = 256
NX = 16384
NY = 2048


def draw_wrapped_phase(key, part):
    keys = jax.random.split(jax.random.fold_in(key, 11), 5)
    row_index = jnp.arange(NX, dtype=jnp.int32)[:, None]
    col_index = jnp.arange(NY, dtype=jnp.int32)[None, :]
    rates = jax.random.randint(keys[0], (2, 2), 1, 17)
    periods = jax.random.randint(keys[1], (2,), 2, 5)
    anchors = jax.random.randint(keys[2], (2,), 0, 64)
    levels = jnp.zeros((NX, NY), jnp.int32)
    for mode in range(2):
        position = (row_index * rates[mode, 0] + col_index * rates[mode, 1]) // 16 + anchors[mode]
        cycle = jnp.remainder(position, 2 * periods[mode])
        levels = levels + jnp.abs(cycle - periods[mode])
    levels = levels + jax.random.randint(keys[3], (NX, NY), 0, 4)
    centred = jnp.remainder(levels, 7) - 3
    jitter = jax.random.uniform(keys[4], (NX, NY), jnp.float32, -0.149, 0.149)
    return centred.astype(jnp.float32) * (2.0 * math.pi / 7.0) + jitter


def setup_inputs(seed: int = 0) -> dict:
    splits = jax.random.split(jax.random.key(seed), 2)
    wrapped_phase = draw_wrapped_phase(jax.random.fold_in(splits[1], 71), 0)
    return dict(wrapped_phase=wrapped_phase)


HIGHEST = lax.Precision.HIGHEST

def wrap_angle(values):
    return jnp.arctan2(jnp.sin(values), jnp.cos(values))

def cosine_table(length):
    frequency = jnp.arange(length, dtype=jnp.float32)[:, None]
    positions = jnp.arange(length, dtype=jnp.float32)[None, :]
    cosine = jnp.cos(math.pi * frequency * (2.0 * positions + 1.0) / (2.0 * length)) * math.sqrt(2.0 / length)
    return jnp.where(frequency == 0.0, cosine * math.sqrt(0.5), cosine)

def solve_tiles(phase_grid):
    length = phase_grid.shape[1]
    down_slope = wrap_angle(phase_grid[:, 1:] - phase_grid[:, :-1])
    zero_row = jnp.zeros_like(phase_grid[:, :1])
    diverge = jnp.concatenate([down_slope, zero_row], 1) - jnp.concatenate([zero_row, down_slope], 1)
    across = wrap_angle(phase_grid[..., 1:] - phase_grid[..., :-1])
    zero_col = jnp.zeros_like(phase_grid[..., :1])
    diverge = diverge + jnp.concatenate([across, zero_col], 3) - jnp.concatenate([zero_col, across], 3)
    cosine = cosine_table(length)
    spectrum = jnp.einsum('pa,rakb,qb->rpkq', cosine, diverge, cosine, precision=HIGHEST)
    frequency = jnp.arange(length, dtype=jnp.float32)
    wave_cos = 2.0 * jnp.cos(math.pi * frequency / length)
    eigenvalue = wave_cos[:, None] + wave_cos[None, :] - 4.0
    corner = frequency[:, None] + frequency[None, :] == 0.0
    safe_eigen = jnp.where(corner, -1.0, eigenvalue)
    scaled = jnp.where(corner[:, None, :], 0.0, spectrum / safe_eigen[:, None, :])
    return jnp.einsum('pa,rpkq,qb->rakb', cosine, scaled, cosine, precision=HIGHEST)

def reference(wrapped_phase):
    tile_rows = NX // TILE
    tile_cols = NY // TILE
    phase_grid = wrapped_phase.reshape(tile_rows, TILE, tile_cols, TILE)
    solved = lax.map(lambda band_tiles: solve_tiles(band_tiles[None])[0], phase_grid)
    east_jump = lax.optimization_barrier(jnp.mean(solved[:, :, :-1, -1] + wrap_angle(phase_grid[:, :, 1:, 0] - phase_grid[:, :, :-1, -1]) - solved[:, :, 1:, 0], axis=1))
    south_jump = lax.optimization_barrier(jnp.mean(solved[:-1, -1, 0, :] + wrap_angle(phase_grid[1:, 0, 0, :] - phase_grid[:-1, -1, 0, :]) - solved[1:, 0, 0, :], axis=1))
    row_starts = jnp.concatenate([jnp.zeros((1,), jnp.float32), jnp.cumsum(south_jump)])
    along_row = jnp.concatenate([jnp.zeros((tile_rows, 1), jnp.float32), jnp.cumsum(east_jump, axis=1)], 1)
    offsets = row_starts[:, None] + along_row
    return (solved + offsets[:, None, :, None]).reshape(NX, NY)
```

```python
import functools
import math

import jax
import jax.numpy as jnp
import numpy as np
from jax import lax
from jax.experimental import pallas as pl
from jax.experimental.pallas import tpu as pltpu
from jax.sharding import PartitionSpec as P

TILE = 256
FULL_TURN = 2.0 * math.pi
MESH = pl.DeviceIdType.MESH
LANES = 128


def wrap_turns(values):
    return values - jnp.round(values)


def cos32(angle):
    return np.cos(angle.astype(np.float64)).astype(np.float32)


def tables(length):
    f32 = np.float32
    order = np.arange(length, dtype=f32)
    angle = (f32(math.pi) * order)[:, None] * (f32(2) * order + f32(1))[None, :] / f32(2 * length)
    cosine = cos32(angle) * f32(math.sqrt(2.0 / length))
    cosine[0] = cosine[0] * f32(math.sqrt(0.5))
    wave = f32(2) * cos32(f32(math.pi) * order / f32(length))
    eigen = (wave[:, None] + wave[None, :]) - f32(4)
    eigen[0, 0] = -1
    inverse = 1.0 / eigen.astype(np.float64)
    inverse[0, 0] = 0
    c64 = cosine.astype(np.float64)
    weights = []
    for cell in (length - 1, 0):
        green = (c64[:, cell] * inverse[0]) @ c64
        step = green - np.append(green[1:], 0.0)
        step[-1] = 0
        weights.append(step / length)
    return cosine, inverse.astype(f32), np.stack(weights).astype(f32)


def split(values):
    high = values.astype(jnp.bfloat16)
    low = (values - high.astype(jnp.float32)).astype(jnp.bfloat16)
    return high, low


def dot(left, right):
    return jnp.dot(left, right, preferred_element_type=jnp.float32)


def stack3(high, low, axis):
    return jnp.concatenate([high, low, high], axis)


BLOCKS = TILE // LANES


def wide(ref, first, rows):
    return jnp.concatenate([ref[first + l, rows, :] for l in range(BLOCKS)], 1)


def put_wide(ref, first, rows, values):
    for l in range(values.shape[1] // LANES):
        ref[first + l, rows, :] = values[:, l * LANES : (l + 1) * LANES]


def in_blocks(table):
    return np.ascontiguousarray(
        table.reshape(table.shape[0], -1, LANES).transpose(1, 0, 2))


def sandwich(pairs, right, left):
    first, second = pl.ds(0, TILE), pl.ds(TILE, TILE)
    table = [wide(right, 0, first), wide(right, 0, first), wide(right, 0, second)]
    table = jnp.concatenate(table, 0)
    inner = [split(dot(stack3(high, low, 1), table)) for high, low in pairs]
    table = [wide(left, 0, first), wide(left, 0, first), wide(left, BLOCKS, first)]
    table = jnp.concatenate(table, 1)
    return [dot(table, stack3(high, low, 0)) for high, low in inner]


def group_size(bands, most):
    return next(g for g in range(most, 0, -1) if bands % g == 0)


def band_rows(i):
    return pl.ds(pl.multiple_of(i * TILE, TILE), TILE)


def band_copy(src, dst, sem, i):
    rows = band_rows(i)
    view = lambda ref: ref.at[rows, :] if len(ref.shape) == 2 else ref.at[:, rows, :]
    return pltpu.make_async_copy(view(src), view(dst), sem.at[i])


def lane_sum(values):
    return jnp.sum(values, axis=1, keepdims=True)


def running(values):
    n = values.shape[0]
    row = lax.broadcasted_iota(jnp.int32, values.shape, 0)
    total = jnp.zeros_like(values)
    for k in range(n - 1):
        total = total + jnp.where(row > k, values[k : k + 1], 0.0)
    return total


CHUNK = 32


def slope_band(x_s, w_ref, i, bands, dh_s, dl_s, sum_s, sum_d, first_s, last_s):
    width = x_s.shape[1]
    base = pl.multiple_of(i * TILE, TILE)
    shape = (CHUNK, width)
    row_id = lax.broadcasted_iota(jnp.int32, shape, 0)
    tile_end = lax.broadcasted_iota(jnp.int32, shape, 1) % TILE == TILE - 1
    fold = lambda v: jnp.sum(v.reshape(CHUNK // 8, 8, v.shape[1]), axis=0)
    acc = jnp.zeros((8, width), jnp.float32)
    acc_last = jnp.zeros((8, TILE), jnp.float32)
    acc_first = jnp.zeros((8, TILE), jnp.float32)
    before = jnp.zeros((1, width), jnp.float32)
    for k in range(TILE // CHUNK):
        rows = pl.ds(base + k * CHUNK, CHUNK)
        x = x_s[rows, :] * (1.0 / FULL_TURN)
        below = pltpu.roll(x, CHUNK - 1, 0)
        if k < TILE // CHUNK - 1:
            below = jnp.where(row_id == CHUNK - 1, x_s[pl.ds(base + (k + 1) * CHUNK, 1), :] * (1.0 / FULL_TURN), below)
        down = wrap_turns(below - x)
        if k == TILE // CHUNK - 1:
            down = jnp.where(row_id == CHUNK - 1, 0.0, down)
        across = wrap_turns(pltpu.roll(x, width - 1, 1) - x)
        acc = acc + fold(across)
        weight = w_ref[k * CHUNK : (k + 1) * CHUNK, 2 * TILE : 2 * TILE + 2]
        acc_last = acc_last + fold(down[:, :TILE] * weight[:, 0:1])
        acc_first = acc_first + fold(down[:, :TILE] * weight[:, 1:2])
        across = jnp.where(tile_end, 0.0, across)
        above = jnp.where(row_id == 0, before, pltpu.roll(down, 1, 0))
        before = down[CHUNK - 1 : CHUNK, :]
        high, low = split(down - above + across - pltpu.roll(across, 1, 1))
        put_wide(dh_s, 0, rows, high)
        put_wide(dl_s, 0, rows, low)
    sum_s[pl.ds(i, 1), :] = jnp.sum(acc, axis=0, keepdims=True)
    sum_d[pl.ds(i, 1), :] = jnp.sum(acc_last, axis=0, keepdims=True)
    sum_d[pl.ds(bands + i, 1), :] = jnp.sum(acc_first, axis=0, keepdims=True)
    first_s[pl.ds(i, 1), :] = x_s[pl.ds(base, 1), 0:TILE]
    last_s[pl.ds(i, 1), :] = x_s[pl.ds(base + TILE - 1, 1), 0:TILE]


def compact(x_s, column):
    height = x_s.shape[0]
    lane = lax.broadcasted_iota(jnp.int32, (8, LANES), 1)
    block = column // LANES * LANES
    rows = []
    for g in range(height // (8 * LANES)):
        acc = jnp.zeros((8, LANES), jnp.float32)
        for k in range(LANES):
            cells = x_s[pl.ds((g * LANES + k) * 8, 8), block : block + LANES]
            acc = jnp.where(lane == k, pltpu.roll(cells, (k - column) % LANES, 1), acc)
        rows.append(acc)
    return jnp.concatenate(rows, 0)


def band_sums(values, bands):
    span = TILE // 8
    row = lax.broadcasted_iota(jnp.int32, (bands, LANES), 0)
    lane = lax.broadcasted_iota(jnp.int32, (bands, LANES), 1)
    per = LANES // span
    sums = jnp.sum(values.reshape(-1, 8, LANES), axis=1)
    picked = jnp.concatenate(
        [jnp.broadcast_to(sums[i // per : i // per + 1], (1, LANES)) for i in range(bands)], 0)
    return lane_sum(jnp.where(lane // span == row % per, picked, 0.0))


def chain_kernel(
    n_row, n_col, x_hbm, w_hbm, left_hbm, right_hbm, left_t_hbm, right_t_hbm, inv_hbm, u_ref, off_ref,
    x_s, w_ref, left, right, left_t, right_t, inv_ref, dh_s, dl_s, sh_s, sl_s,
    col_out, col_in, top_out, top_in, sum_s, sum_d, first_s, last_s,
    down_out, down_in, row_out, row_in,
    edge_send, edge_recv, down_send, down_recv, row_send, row_recv,
    x_sem, table_sem,
):
    r, c = lax.axis_index("row"), lax.axis_index("col")
    height, width = x_s.shape
    bands, tiles = height // TILE, width // TILE
    band_copy(x_hbm, x_s, x_sem, 0).start()
    tables = [(w_hbm, w_ref), (right_hbm, right), (left_hbm, left), (inv_hbm, inv_ref),
              (right_t_hbm, right_t), (left_t_hbm, left_t)]
    tables = [pltpu.make_async_copy(a, b, table_sem.at[k]) for k, (a, b) in enumerate(tables)]
    tables[0].start()
    for i in range(1, bands):
        band_copy(x_hbm, x_s, x_sem, i).start()
    for copy in tables[1:]:
        copy.start()

    barrier = pltpu.get_barrier_semaphore()

    def greet(row, col):
        pl.semaphore_signal(barrier, inc=1, device_id=(row, col), device_id_type=MESH)

    def greet_above(k, carry):
        greet(k, 0)
        return carry

    def greet_left(k, carry):
        greet(r, k)
        return carry

    lax.fori_loop(0, r, greet_above, 0)
    lax.fori_loop(0, c, greet_left, 0)
    is_first = c == 0
    has_right = c < n_col - 1
    has_below = r < n_row - 1
    pl.when(has_right)(lambda: greet(r, c + 1))
    pl.when(jnp.logical_and(is_first, has_below))(lambda: greet(r + 1, 0))

    def slopes(i):
        slope_band(x_s, w_ref, i, bands, dh_s, dl_s, sum_s, sum_d, first_s, last_s)

    def forward(bands_):
        places = [(i, t) for i in bands_ for t in range(tiles)]
        pairs = [
            (wide(dh_s, t * BLOCKS, band_rows(i)), wide(dl_s, t * BLOCKS, band_rows(i)))
            for i, t in places
        ]
        for (i, t), spectrum in zip(places, sandwich(pairs, right, left)):
            high, low = split(spectrum * inv_ref[...])
            put_wide(sh_s, t * BLOCKS, band_rows(i), high)
            put_wide(sl_s, t * BLOCKS, band_rows(i), low)

    def backward(bands_):
        places = [(i, t) for i in bands_ for t in range(tiles)]
        pairs = [
            (wide(sh_s, t * BLOCKS, band_rows(i)), wide(sl_s, t * BLOCKS, band_rows(i)))
            for i, t in places
        ]
        for (i, t), solved in zip(places, sandwich(pairs, right_t, left_t)):
            u_ref[band_rows(i), t * TILE : (t + 1) * TILE] = solved

    band_copy(x_hbm, x_s, x_sem, 0).wait()
    tables[0].wait()
    slopes(0)
    for i in range(1, bands):
        band_copy(x_hbm, x_s, x_sem, i).wait()
    for copy in tables[1:]:
        copy.wait()
    col_out[...] = compact(x_s, 0)
    top_out[...] = jnp.broadcast_to(x_s[0:1, 0:TILE], top_out.shape)

    peers = (n_col - 1 - c) + jnp.where(is_first, 0, 1)
    peers = peers + jnp.where(is_first, (n_row - 1 - r) * n_col + jnp.where(r > 0, 1, 0), 0)
    pl.semaphore_wait(barrier, peers)
    edge_col = pltpu.make_async_remote_copy(
        src_ref=col_out, dst_ref=col_in, send_sem=edge_send.at[0], recv_sem=edge_recv.at[0],
        device_id=(r, jnp.maximum(c - 1, 0)), device_id_type=MESH)
    edge_top = pltpu.make_async_remote_copy(
        src_ref=top_out, dst_ref=top_in, send_sem=edge_send.at[1], recv_sem=edge_recv.at[1],
        device_id=(jnp.maximum(r - 1, 0), c), device_id_type=MESH)
    send_top = jnp.logical_and(is_first, r > 0)
    pl.when(jnp.logical_not(is_first))(lambda: edge_col.start())
    pl.when(send_top)(lambda: edge_top.start())

    last_col = compact(x_s, width - 1)
    for i in range(1, bands):
        slopes(i)
        if i % 2 == 1:
            forward([i - 1, i])

    scale = FULL_TURN / TILE
    sums = sum_s[...]
    last_w, first_w = w_ref[0:1, 0:TILE], w_ref[0:1, TILE : 2 * TILE]
    lasts = [lane_sum(sums[:, t * TILE : (t + 1) * TILE] * last_w) for t in range(tiles)]
    firsts = [lane_sum(sums[:, t * TILE : (t + 1) * TILE] * first_w) for t in range(tiles)]
    along = [jnp.zeros((bands, 1), jnp.float32)]
    for t in range(tiles - 1):
        end = (t + 1) * TILE
        along.append(along[-1] + lasts[t] + sums[:, end - 1 : end] * scale - firsts[t + 1])
    down_last = lane_sum(sum_d[0:bands, :])
    down_first = lane_sum(sum_d[bands : 2 * bands, :])
    down_first0 = down_first[0:1]

    down_copy = lambda row, col: pltpu.make_async_remote_copy(
        src_ref=down_out, dst_ref=down_in.at[r], send_sem=down_send, recv_sem=down_recv.at[r],
        device_id=(row, col), device_id_type=MESH)
    row_copy = lambda k: pltpu.make_async_remote_copy(
        src_ref=row_out, dst_ref=row_in.at[c], send_sem=row_send, recv_sem=row_recv.at[c],
        device_id=(r, k), device_id_type=MESH)

    pl.when(jnp.logical_and(is_first, has_below))(lambda: edge_top.wait_recv())
    below = jnp.concatenate([first_s[1:bands, :], top_in[0:1, :]], 0)
    border = lane_sum(wrap_turns((below - last_s[0:bands, :]) * (1.0 / FULL_TURN))) * scale
    next_first = jnp.concatenate([down_first[1:bands], down_first[0:1]], 0)
    jump = down_last + border - next_first
    jump_total = jnp.sum(jump, axis=0, keepdims=True)
    starts = running(jump) - jnp.where(r > 0, down_first0, 0.0)
    lane = lax.broadcasted_iota(jnp.int32, (8, LANES), 1)
    down_out[...] = jnp.where(lane == 0, jump_total, jnp.where(lane == 1, down_first0, 0.0))
    n_down = jnp.where(is_first, (n_row - 1 - r) * n_col, 0)

    def send_down(k, carry):
        down_copy(r + 1 + k // n_col, k % n_col).start()
        return carry

    lax.fori_loop(0, n_down, send_down, 0)

    pl.when(has_right)(lambda: edge_col.wait_recv())
    edge = wrap_turns((col_in[...] - last_col) * (1.0 / FULL_TURN))
    row_total = along[-1] + lasts[-1] + band_sums(edge, bands) * scale - firsts[0]
    lane = lax.broadcasted_iota(jnp.int32, (bands, LANES), 1)
    row_out[...] = jnp.where(
        lane == 0, row_total, jnp.where(lane == 1, starts + firsts[0], 0.0))

    def send_row(k, carry):
        row_copy(k).start()
        return carry

    lax.fori_loop(c + 1, n_col, send_row, 0)

    for j in range(bands // 4):
        backward([4 * j + k for k in range(4)])

    pl.when(jnp.logical_not(is_first))(lambda: edge_col.wait_send())
    pl.when(send_top)(lambda: edge_top.wait_send())

    def sent_down(k, carry):
        down_copy(r + 1 + k // n_col, k % n_col).wait_send()
        return carry

    lax.fori_loop(0, n_down, sent_down, 0)

    def sent_row(k, carry):
        row_copy(k).wait_send()
        return carry

    lax.fori_loop(c + 1, n_col, sent_row, 0)

    above = jnp.zeros((1, 1), jnp.float32)
    for k in range(n_row - 1):
        pl.when(k < r)(lambda: pltpu.make_async_remote_copy(
            src_ref=down_out, dst_ref=down_in.at[k], send_sem=down_send, recv_sem=down_recv.at[k],
            device_id=(r, c), device_id_type=MESH).wait_recv())
        above = above + jnp.where(k < r, down_in[k, 0:1, 0:1], 0.0)
    above = above + jnp.where(r > 0, down_in[0, 0:1, 1:2], 0.0)
    offset = jnp.where(is_first, starts, -firsts[0]) + above
    for k in range(n_col - 1):
        pl.when(k < c)(lambda: pltpu.make_async_remote_copy(
            src_ref=row_out, dst_ref=row_in.at[k], send_sem=row_send, recv_sem=row_recv.at[k],
            device_id=(r, c), device_id_type=MESH).wait_recv())
        offset = offset + jnp.where(k < c, row_in[k, :, 0:1], 0.0)
    offset = offset + jnp.where(c > 0, row_in[0, :, 1:2], 0.0)
    for t in range(tiles):
        off_ref[:, t * TILE : (t + 1) * TILE] = jnp.broadcast_to(offset + along[t], (bands, TILE))


def finish_kernel(u_ref, off_ref, out_hbm, out_s, out_sem):
    height, width = out_s.shape
    bands = height // TILE
    for i in range(bands):
        rows = band_rows(i)
        out_s[rows, :] = u_ref[rows, :] + off_ref[i : i + 1, :]
        band_copy(out_s, out_hbm, out_sem, i).start()
    for i in range(bands):
        band_copy(out_s, out_hbm, out_sem, i).wait()


def per_device(n_row, n_col, x):
    height, width = x.shape
    bands = height // TILE
    blocks = (width // LANES, height, LANES)
    cosine, inverse, weights = tables(TILE)
    high = cosine.astype(jnp.bfloat16)
    low = (cosine - high.astype(np.float32)).astype(jnp.bfloat16)
    beside = in_blocks(np.concatenate([high, low], 1))
    over = in_blocks(np.concatenate([high, low], 0))
    beside_t = in_blocks(np.concatenate([high.T, low.T], 1))
    over_t = in_blocks(np.concatenate([high.T, low.T], 0))
    w = np.zeros((TILE, 2 * TILE + LANES), np.float32)
    weights = weights * np.float32(FULL_TURN)
    w[:, 0:TILE] = weights[0]
    w[:, TILE : 2 * TILE] = weights[1]
    w[:, 2 * TILE] = weights[0]
    w[:, 2 * TILE + 1] = weights[1]

    vmem = pl.BlockSpec(memory_space=pltpu.VMEM)
    hbm = pl.BlockSpec(memory_space=pltpu.HBM)
    f32, bf16 = jnp.float32, jnp.bfloat16
    consts = [w, beside, over_t, beside_t, over, inverse * np.float32(FULL_TURN)]
    u, offsets = pl.pallas_call(
        functools.partial(chain_kernel, n_row, n_col),
        out_shape=[pltpu.VMEM(x.shape, f32), pltpu.VMEM((bands, width), f32)],
        in_specs=[hbm] * 7,
        out_specs=[vmem, vmem],
        scratch_shapes=[pltpu.VMEM((height, width), f32)]
        + [pltpu.VMEM(t.shape, t.dtype) for t in consts]
        + [
            pltpu.VMEM(blocks, bf16),
            pltpu.VMEM(blocks, bf16),
            pltpu.VMEM(blocks, bf16),
            pltpu.VMEM(blocks, bf16),
            pltpu.VMEM((height // LANES, LANES), f32),
            pltpu.VMEM((height // LANES, LANES), f32),
            pltpu.VMEM((8, TILE), f32),
            pltpu.VMEM((8, TILE), f32),
            pltpu.VMEM((bands, width), f32),
            pltpu.VMEM((2 * bands, TILE), f32),
            pltpu.VMEM((bands, TILE), f32),
            pltpu.VMEM((2 * bands, TILE), f32),
            pltpu.VMEM((8, LANES), f32),
            pltpu.VMEM((n_row - 1, 8, LANES), f32),
            pltpu.VMEM((bands, LANES), f32),
            pltpu.VMEM((n_col - 1, bands, LANES), f32),
            pltpu.SemaphoreType.DMA((2,)),
            pltpu.SemaphoreType.DMA((2,)),
            pltpu.SemaphoreType.DMA,
            pltpu.SemaphoreType.DMA((n_row - 1,)),
            pltpu.SemaphoreType.DMA,
            pltpu.SemaphoreType.DMA((n_col - 1,)),
            pltpu.SemaphoreType.DMA((bands,)),
            pltpu.SemaphoreType.DMA((len(consts),)),
        ],
        compiler_params=pltpu.CompilerParams(
            collective_id=0, has_side_effects=True, vmem_limit_bytes=59 << 20),
        name="chain",
    )(x, *[jnp.asarray(t) for t in consts])

    return pl.pallas_call(
        finish_kernel,
        out_shape=jax.ShapeDtypeStruct(x.shape, f32),
        in_specs=[vmem, vmem],
        out_specs=hbm,
        scratch_shapes=[
            pltpu.VMEM((height, width), f32),
            pltpu.SemaphoreType.DMA((bands,)),
        ],
        compiler_params=pltpu.CompilerParams(vmem_limit_bytes=16 << 20),
        name="finish",
    )(u, offsets)


def solution(mesh):
    n_row, n_col = mesh.shape["row"], mesh.shape["col"]
    return jax.shard_map(
        functools.partial(per_device, n_row, n_col), mesh=mesh,
        in_specs=(P("row", "col"),), out_specs=P("row", "col"), check_vma=False,
    )
```

```python
import functools
import math

import jax
import jax.numpy as jnp
import numpy as np
from jax import lax
from jax.experimental import pallas as pl
from jax.experimental.pallas import tpu as pltpu
from jax.sharding import PartitionSpec as P

TILE = 256
FULL_TURN = 2.0 * math.pi
MESH = pl.DeviceIdType.MESH
LANES = 128


def wrap_turns(values):
    return values - jnp.round(values)


def cos32(angle):
    return np.cos(angle.astype(np.float64)).astype(np.float32)


def tables(length):
    f32 = np.float32
    order = np.arange(length, dtype=f32)
    angle = (f32(math.pi) * order)[:, None] * (f32(2) * order + f32(1))[None, :] / f32(2 * length)
    cosine = cos32(angle) * f32(math.sqrt(2.0 / length))
    cosine[0] = cosine[0] * f32(math.sqrt(0.5))
    wave = f32(2) * cos32(f32(math.pi) * order / f32(length))
    eigen = (wave[:, None] + wave[None, :]) - f32(4)
    eigen[0, 0] = -1
    inverse = 1.0 / eigen.astype(np.float64)
    inverse[0, 0] = 0
    c64 = cosine.astype(np.float64)
    weights = []
    for cell in (length - 1, 0):
        green = (c64[:, cell] * inverse[0]) @ c64
        step = green - np.append(green[1:], 0.0)
        step[-1] = 0
        weights.append(step / length)
    return cosine, inverse.astype(f32), np.stack(weights).astype(f32)


def split(values):
    high = values.astype(jnp.bfloat16)
    low = (values - high.astype(jnp.float32)).astype(jnp.bfloat16)
    return high, low


def dot(left, right):
    return jnp.dot(left, right, preferred_element_type=jnp.float32)


def stack3(high, low, axis):
    return jnp.concatenate([high, low, high], axis)


BLOCKS = TILE // LANES


def wide(ref, first, rows):
    return jnp.concatenate([ref[first + l, rows, :] for l in range(BLOCKS)], 1)


def put_wide(ref, first, rows, values):
    for l in range(values.shape[1] // LANES):
        ref[first + l, rows, :] = values[:, l * LANES : (l + 1) * LANES]


def in_blocks(table):
    return np.ascontiguousarray(
        table.reshape(table.shape[0], -1, LANES).transpose(1, 0, 2))


def sandwich(pairs, right, left):
    first, second = pl.ds(0, TILE), pl.ds(TILE, TILE)
    table = [wide(right, 0, first), wide(right, 0, first), wide(right, 0, second)]
    table = jnp.concatenate(table, 0)
    inner = [split(dot(stack3(high, low, 1), table)) for high, low in pairs]
    table = [wide(left, 0, first), wide(left, 0, first), wide(left, BLOCKS, first)]
    table = jnp.concatenate(table, 1)
    return [dot(table, stack3(high, low, 0)) for high, low in inner]


def group_size(bands, most):
    return next(g for g in range(most, 0, -1) if bands % g == 0)


def band_rows(i):
    return pl.ds(pl.multiple_of(i * TILE, TILE), TILE)


def band_copy(src, dst, sem, i):
    rows = band_rows(i)
    view = lambda ref: ref.at[rows, :] if len(ref.shape) == 2 else ref.at[:, rows, :]
    return pltpu.make_async_copy(view(src), view(dst), sem.at[i])


def lane_sum(values):
    return jnp.sum(values, axis=1, keepdims=True)


def running(values):
    n = values.shape[0]
    row = lax.broadcasted_iota(jnp.int32, values.shape, 0)
    total = jnp.zeros_like(values)
    for k in range(n - 1):
        total = total + jnp.where(row > k, values[k : k + 1], 0.0)
    return total


def band_sums(values, bands):
    span = TILE // 8
    row = lax.broadcasted_iota(jnp.int32, (bands, LANES), 0)
    lane = lax.broadcasted_iota(jnp.int32, (bands, LANES), 1)
    per = LANES // span
    sums = jnp.sum(values.reshape(-1, 8, LANES), axis=1)
    picked = jnp.concatenate(
        [jnp.broadcast_to(sums[i // per : i // per + 1], (1, LANES)) for i in range(bands)], 0)
    return lane_sum(jnp.where(lane // span == row % per, picked, 0.0))


LOW = 8
STEP = 16
SPAN = 32


def low_tables(length, bands):
    order = np.arange(length, dtype=np.float64)
    exact = np.cos(np.pi * order[:, None] * (2 * order + 1) / (2 * length)) * math.sqrt(2.0 / length)
    exact[0] *= math.sqrt(0.5)
    wave = 2 * np.cos(np.pi * order / length)
    eigen = wave[:, None] + wave[None, :] - 4
    inverse = tables(length)[1].astype(np.float64)
    change = (eigen * inverse - 1)[:LOW, :LOW]
    change[0, 0] = 0
    means = exact[:LOW].reshape(LOW, length // SPAN, SPAN // 8, 8).mean(2).reshape(LOW, -1)
    full = np.zeros((bands * LOW, LANES), np.float32)
    full[:, :LOW] = np.tile(change, (bands, 1))
    return np.kron(np.eye(bands), means).astype(np.float32), full


def slope_band(x_s, wl_ref, wf_ref, step_ref, net_ref, i, d_s, xb_s, cols_s, sum_x, sum_n, sum_l, sum_f):
    blocks = x_s.shape[0]
    base = pl.multiple_of(i * TILE, TILE) + 8
    shape = (STEP, LANES)
    row = lax.broadcasted_iota(jnp.int32, shape, 0)
    lane8 = lax.broadcasted_iota(jnp.int32, (8, LANES), 1)
    bottom, top = row == STEP - 1, row == 0
    f32, bf16 = jnp.float32, jnp.bfloat16
    none = jnp.zeros(shape, bf16)
    zero = jnp.zeros((8, LANES), f32)
    fold = lambda v: v[0:8] + v[8:16]
    counts = lambda v: jnp.round(v * bf16(1.0 / FULL_TURN))
    groups = range(0, TILE, STEP)
    near = [x_s[l, pl.ds(base, TILE), :].astype(bf16) for l in range(blocks)]
    nets, totals = [], []
    for t in range(blocks // BLOCKS):
        some = near[t * BLOCKS : (t + 2) * BLOCKS]
        n = dot(jnp.concatenate(some, 1), step_ref[0 : len(some) * LANES, :])
        n = counts(n.astype(bf16))
        totals.append(functools.reduce(jnp.add, [n[g : g + STEP] for g in groups]))
        nets.append(dot(n, net_ref[...]).astype(bf16))
    acc_x = [zero] * blocks
    acc_l, acc_f = zero, zero
    first, last = zero, zero
    part = [None] * blocks
    halves = [None] * blocks
    for g in groups:
        x = [x_s[l, pl.ds(base + g, STEP), :] for l in range(blocks)]
        tall, whole = [], []
        for l in range(blocks):
            if g == TILE - STEP:
                below = jnp.where(bottom, x[l], pltpu.roll(x[l], STEP - 1, 0))
            else:
                below = x_s[l, pl.ds(base + g + 1, STEP), :]
            above = x_s[l, pl.ds(base + g - 1, STEP), :]
            mine = near[l][g : g + STEP]
            down = counts(below.astype(bf16) - mine)
            up = counts(mine - above.astype(bf16))
            if g == 0:
                up = jnp.where(top, none, up)
            if l < BLOCKS:
                tall.append(below - x[l])
                whole.append(down)
            net = nets[l // BLOCKS][g : g + STEP, l % BLOCKS * LANES : (l % BLOCKS + 1) * LANES]
            d_s[l, pl.ds(base - 8 + g, STEP), :] = net + (down - up)
            half = fold(x[l])
            if g % SPAN == 0:
                part[l] = half
            else:
                total = part[l] + half
                acc_x[l] = acc_x[l] + total
                if g % (2 * SPAN) == STEP:
                    halves[l] = total
                else:
                    xb_s[l, pl.ds(pl.multiple_of(i * (TILE // 4), 16) + g // (2 * SPAN) * 16, 16), :] = (
                        jnp.concatenate([halves[l], total], 0).astype(bf16))
        slope = functools.reduce(jnp.add, tall) * (1.0 / FULL_TURN)
        slope = slope - functools.reduce(jnp.add, whole).astype(f32)
        acc_l = acc_l + fold(slope * wl_ref[g : g + STEP, :])
        acc_f = acc_f + fold(slope * wf_ref[g : g + STEP, :])
        for j in range(STEP // 8):
            k = g // 8 + j
            cells = slice(8 * j, 8 * j + 8)
            first = jnp.where(lane8 == k, pltpu.roll(x[0][cells], k, 1) if k else x[0][cells], first)
            last = jnp.where(lane8 == k, pltpu.roll(x[-1][cells], k + 1, 1), last)
    here = pl.ds(pl.multiple_of(i * 8, 8), 8)
    cols_s[0, here, :] = first
    cols_s[1, here, :] = last
    sum_x[pl.ds(i, 1), :] = jnp.sum(jnp.concatenate(acc_x, 1), axis=0, keepdims=True)
    sum_n[pl.ds(i, 1), :] = jnp.sum(jnp.concatenate(totals, 1).astype(f32), axis=0, keepdims=True)
    sum_l[pl.ds(i, 1), :] = jnp.sum(acc_l, axis=0, keepdims=True)
    sum_f[pl.ds(i, 1), :] = jnp.sum(acc_f, axis=0, keepdims=True)


def gather_cols(cols_s, side, bands):
    span = TILE // 8
    per = LANES // span
    rows = []
    for g in range(0, bands, per):
        parts = [cols_s[side, (g + j) * 8 : (g + j + 1) * 8, :] for j in range(per)]
        parts = [pltpu.roll(v, j * span, 1) if j else v for j, v in enumerate(parts)]
        rows.append(functools.reduce(jnp.add, parts))
    return jnp.concatenate(rows, 0)


def chain_kernel(
    n_row, n_col, x_hbm, step_hbm, net_hbm, wl_hbm, wf_hbm, w_hbm, left_hbm, right_hbm, left_t_hbm, right_t_hbm, inv_hbm,
    low_hbm, change_hbm, u_ref, off_ref,
    x_s, step_ref, net_ref, wl_ref, wf_ref, w_ref, left, right, left_t, right_t, inv_ref, low_ref, change_ref,
    d_s, xb_s, cols_s, corr_s, sum_x, sum_n, sum_l, sum_f,
    col_out, col_in, down_out, down_in, row_out, row_in,
    edge_send, edge_recv, down_send, down_recv, row_send, row_recv,
    x_sem, table_sem,
):
    r, c = lax.axis_index("row"), lax.axis_index("col")
    blocks, height = x_s.shape[0], x_s.shape[1] - 16
    bands, tiles = height // TILE, blocks // BLOCKS

    def x_copy(i, l):
        return pltpu.make_async_copy(
            x_hbm.at[band_rows(i), l * LANES : (l + 1) * LANES], x_s.at[l, pl.ds(pl.multiple_of(i * TILE, TILE) + 8, TILE), :],
            x_sem.at[i, l])

    def fetch(i, carry):
        for l in range(blocks):
            x_copy(i, l).start()
        return carry

    def arrive(i):
        for l in range(blocks):
            x_copy(i, l).wait()

    copies = [(step_hbm, step_ref), (net_hbm, net_ref), (wl_hbm, wl_ref), (wf_hbm, wf_ref), (w_hbm, w_ref), (right_hbm, right), (left_hbm, left),
              (inv_hbm, inv_ref), (low_hbm, low_ref), (change_hbm, change_ref),
              (right_t_hbm, right_t), (left_t_hbm, left_t)]
    copies = [pltpu.make_async_copy(a, b, table_sem.at[k]) for k, (a, b) in enumerate(copies)]
    fetch(0, 0)
    for copy in copies[:4]:
        copy.start()
    lax.fori_loop(1, bands, fetch, 0)
    for copy in copies[4:]:
        copy.start()

    barrier = pltpu.get_barrier_semaphore()

    def greet(row, col):
        pl.semaphore_signal(barrier, inc=1, device_id=(row, col), device_id_type=MESH)

    def greet_above(k, carry):
        greet(k, 0)
        return carry

    def greet_left(k, carry):
        greet(r, k)
        return carry

    is_first = c == 0
    has_right = c < n_col - 1
    lax.fori_loop(0, r, greet_above, 0)
    lax.fori_loop(0, c, greet_left, 0)
    pl.when(has_right)(lambda: greet(r, c + 1))

    pair = group_size(bands, 2)

    def slopes(j, carry):
        for k in range(pair):
            arrive(j * pair + k)
        for k in range(pair):
            slope_band(x_s, wl_ref, wf_ref, step_ref, net_ref, j * pair + k,
                       d_s, xb_s, cols_s, sum_x, sum_n, sum_l, sum_f)
        return carry

    for copy in copies[:4]:
        copy.wait()
    lax.fori_loop(0, bands // pair, slopes, 0)
    col_out[...] = gather_cols(cols_s, 0, bands)
    edge_col = pltpu.make_async_remote_copy(
        src_ref=col_out, dst_ref=col_in, send_sem=edge_send, recv_sem=edge_recv,
        device_id=(r, jnp.maximum(c - 1, 0)), device_id_type=MESH)

    @pl.when(jnp.logical_not(is_first))
    def _():
        pl.semaphore_wait(barrier, n_col - c)
        edge_col.start()

    scale = FULL_TURN / TILE
    down_last = lane_sum(sum_l[...])
    down_first = lane_sum(sum_f[...])
    border = jnp.zeros((bands - 1, LANES), jnp.float32)
    for l in range(BLOCKS):
        ends = [x_s[l, i * TILE + 7 : i * TILE + 9, :] for i in range(1, bands)]
        ends = [v[1:2] - v[0:1] for v in ends]
        border = border + wrap_turns(jnp.concatenate(ends, 0) * (1.0 / FULL_TURN))
    border = lane_sum(border) * scale
    zero = jnp.zeros((1, 1), jnp.float32)
    jump = down_last + jnp.concatenate([border - down_first[1:bands], zero], 0)
    jump_total = jnp.sum(jump, axis=0, keepdims=True) - down_first[0:1]
    starts = running(jump)
    starts = starts - jnp.where(r > 0, down_first[0:1], 0.0)
    lane = lax.broadcasted_iota(jnp.int32, (1, LANES), 1)
    tops = [x_s[l, 8:9, :] for l in range(BLOCKS)]
    scalars = jnp.where(lane == 0, jump_total, jnp.where(lane == 1, down_first[0:1], 0.0))
    down_out[...] = jnp.concatenate(
        tops + [x_s[l, height + 7 : height + 8, :] for l in range(BLOCKS)] + [scalars], 0)

    down_copy = lambda row, col: pltpu.make_async_remote_copy(
        src_ref=down_out, dst_ref=down_in.at[r], send_sem=down_send, recv_sem=down_recv.at[r],
        device_id=(row, col), device_id_type=MESH)
    row_copy = lambda k: pltpu.make_async_remote_copy(
        src_ref=row_out, dst_ref=row_in.at[c], send_sem=row_send, recv_sem=row_recv.at[c],
        device_id=(r, k), device_id_type=MESH)
    for copy in copies[4:]:
        copy.wait()
    first, second = pl.ds(0, TILE), pl.ds(TILE, TILE)
    for t in range(tiles):
        low = jnp.concatenate([xb_s[t * BLOCKS + k] for k in range(BLOCKS)], 1)
        low = dot(low, right[0, first, :]).astype(jnp.bfloat16)
        corr_s[t] = dot(low_ref[...], low) * change_ref[...]

    def solve(some):
        places = [(i, t) for i in some for t in range(tiles)]
        table = jnp.concatenate([wide(right, 0, first), wide(right, 0, second)], 0)
        data = [wide(d_s, t * BLOCKS, band_rows(i)) for i, t in places]
        inner = [split(dot(jnp.concatenate([d, d], 1), table)) for d in data]
        table = [wide(left, 0, first), wide(left, 0, first), wide(left, BLOCKS, first)]
        table = jnp.concatenate(table, 1)
        pairs = []
        for (i, t), (high, low) in zip(places, inner):
            scaled = dot(table, stack3(high, low, 0)) * inv_ref[...]
            corner = scaled[0:LOW, 0:LANES] + corr_s[t, i * LOW : (i + 1) * LOW, :]
            scaled = jnp.concatenate(
                [jnp.concatenate([corner, scaled[0:LOW, LANES:]], 1), scaled[LOW:]], 0)
            pairs.append(split(scaled))
        for (i, t), solved in zip(places, sandwich(pairs, right_t, left_t)):
            u_ref[band_rows(i), t * TILE : (t + 1) * TILE] = (
                solved + wide(x_s, t * BLOCKS, pl.ds(i * TILE + 8, TILE)))

    solve(range(0, 2))

    def each_below(act):
        def per_row(k, carry):
            def per_col(j, carry):
                act(down_copy(n_row - 1 - k, n_col - 1 - j))
                return carry
            return lax.fori_loop(0, n_col, per_col, carry)
        lax.fori_loop(0, jnp.where(is_first, n_row - 1 - r, 0), per_row, 0)

    @pl.when(is_first)
    def _():
        pl.semaphore_wait(barrier, (n_row - 1 - r) * n_col + n_col - 1)

    each_below(lambda copy: copy.start())

    last_col = gather_cols(cols_s, 1, bands)
    sums = sum_x[...]
    mean = [lane_sum(sums[:, t * TILE : (t + 1) * TILE]) * (1.0 / TILE / TILE) for t in range(tiles)]
    sums = (pltpu.roll(sums, blocks * LANES - 1, 1) - sums) * (1.0 / FULL_TURN) - sum_n[...]
    last_w, first_w = w_ref[0:1, 0:TILE], w_ref[0:1, TILE : 2 * TILE]
    lasts = [lane_sum(sums[:, t * TILE : (t + 1) * TILE] * last_w) for t in range(tiles)]
    firsts = [lane_sum(sums[:, t * TILE : (t + 1) * TILE] * first_w) for t in range(tiles)]
    along = [jnp.zeros((bands, 1), jnp.float32)]
    for t in range(tiles - 1):
        end = (t + 1) * TILE
        along.append(along[-1] + lasts[t] + sums[:, end - 1 : end] * scale - firsts[t + 1])

    pl.when(has_right)(lambda: edge_col.wait_recv())
    edge = wrap_turns((col_in[...] - last_col) * (1.0 / FULL_TURN))
    row_total = along[-1] + lasts[-1] + band_sums(edge, bands) * scale - firsts[0]
    lane = lax.broadcasted_iota(jnp.int32, (bands, LANES), 1)
    row_out[0:bands, :] = jnp.where(
        lane == 0, row_total, jnp.where(lane == 1, starts + firsts[0], 0.0))
    row_out[bands : bands + BLOCKS, :] = jnp.concatenate(tops, 0)

    def send_row(k, carry):
        row_copy(k).start()
        return carry

    lax.fori_loop(c + 1, n_col, send_row, 0)

    for k in range(2, bands, 3):
        solve(range(k, min(k + 3, bands)))

    pl.when(jnp.logical_not(is_first))(lambda: edge_col.wait_send())

    each_below(lambda copy: copy.wait_send())

    def sent_row(k, carry):
        row_copy(k).wait_send()
        return carry

    lax.fori_loop(c + 1, n_col, sent_row, 0)

    offset = jnp.where(is_first, starts, -firsts[0])
    for k in range(n_col - 1):
        pl.when(k < c)(lambda: pltpu.make_async_remote_copy(
            src_ref=row_out, dst_ref=row_in.at[k], send_sem=row_send, recv_sem=row_recv.at[k],
            device_id=(r, c), device_id_type=MESH).wait_recv())
        offset = offset + jnp.where(k < c, row_in[k, 0:bands, 0:1], 0.0)
    offset = offset + jnp.where(c > 0, row_in[0, 0:bands, 1:2], 0.0)

    for k in range(n_row - 1):
        pl.when(k < r)(lambda: pltpu.make_async_remote_copy(
            src_ref=down_out, dst_ref=down_in.at[k], send_sem=down_send, recv_sem=down_recv.at[k],
            device_id=(r, c), device_id_type=MESH).wait_recv())
    edge = jnp.zeros((n_row - 1, LANES), jnp.float32)
    number = lax.broadcasted_iota(jnp.int32, (n_row - 1, LANES), 0)
    for l in range(BLOCKS):
        own = jnp.where(is_first, tops[l], row_in[0, bands + l : bands + l + 1, :])
        upper = jnp.concatenate([down_in[k, BLOCKS + l : BLOCKS + l + 1, :] for k in range(n_row - 1)], 0)
        lower = jnp.concatenate([down_in[k, l : l + 1, :] for k in range(1, n_row - 1)] + [own], 0)
        lower = jnp.where(number == r - 1, own, lower)
        edge = edge + wrap_turns((lower - upper) * (1.0 / FULL_TURN))
    single = jnp.concatenate([down_in[k, 2 * BLOCKS : 2 * BLOCKS + 1, :] for k in range(n_row - 1)], 0)
    lane = lax.broadcasted_iota(jnp.int32, (n_row - 1, LANES), 1)
    pick = jnp.where(lane == 0, single, 0.0) + jnp.where((lane == 1) & (number == 0), single, 0.0)
    above = jnp.where(number < r, edge * scale + pick, 0.0)
    above = lane_sum(jnp.sum(above, axis=0, keepdims=True))
    offset = offset + above
    for t in range(tiles):
        off_ref[:, t * TILE : (t + 1) * TILE] = jnp.broadcast_to(
            offset + along[t] - mean[t], (bands, TILE))


def finish_kernel(u_ref, off_ref, out_hbm, out_s, out_sem):
    height, width = out_s.shape
    bands = height // TILE
    for i in range(bands):
        rows = band_rows(i)
        out_s[rows, :] = u_ref[rows, :] + off_ref[i : i + 1, :]
        band_copy(out_s, out_hbm, out_sem, i).start()
    for i in range(bands):
        band_copy(out_s, out_hbm, out_sem, i).wait()


def per_device(n_row, n_col, x):
    height, width = x.shape
    bands = height // TILE
    blocks = width // LANES
    tiles = width // TILE
    cosine, inverse, weights = tables(TILE)
    high = cosine.astype(jnp.bfloat16)
    low = (cosine - high.astype(np.float32)).astype(jnp.bfloat16)
    beside = in_blocks(np.concatenate([high, low], 1))
    over = in_blocks(np.concatenate([high, low], 0))
    beside_t = in_blocks(np.concatenate([high.T, low.T], 1))
    over_t = in_blocks(np.concatenate([high.T, low.T], 0))
    weights = weights * np.float32(FULL_TURN)
    w = np.tile(weights.reshape(1, -1), (8, 1))
    wl = np.ascontiguousarray(np.broadcast_to(weights[0][:, None], (TILE, LANES)))
    wf = np.ascontiguousarray(np.broadcast_to(weights[1][:, None], (TILE, LANES)))
    means, change = low_tables(TILE, bands)
    eye = np.eye(2 * TILE, TILE, dtype=np.float32)
    step = np.eye(2 * TILE, TILE, -1, dtype=np.float32) - eye
    net = np.eye(TILE, dtype=np.float32) - np.eye(TILE, k=1, dtype=np.float32)
    net[TILE - 1] = 0

    vmem = pl.BlockSpec(memory_space=pltpu.VMEM)
    hbm = pl.BlockSpec(memory_space=pltpu.HBM)
    f32, bf16 = jnp.float32, jnp.bfloat16
    consts = [step.astype(bf16), net.astype(bf16), wl, wf, w, beside, over_t, beside_t, over, inverse * np.float32(-FULL_TURN),
              means.astype(bf16), change]
    u, offsets = pl.pallas_call(
        functools.partial(chain_kernel, n_row, n_col),
        out_shape=[pltpu.VMEM(x.shape, f32), pltpu.VMEM((bands, width), f32)],
        in_specs=[hbm] * (1 + len(consts)),
        out_specs=[vmem, vmem],
        scratch_shapes=[pltpu.VMEM((blocks, height + 16, LANES), f32)]
        + [pltpu.VMEM(t.shape, t.dtype) for t in consts]
        + [
            pltpu.VMEM((blocks, height, LANES), bf16),
            pltpu.VMEM((blocks, height // 4, LANES), bf16),
            pltpu.VMEM((2, bands * 8, LANES), f32),
            pltpu.VMEM((tiles, bands * LOW, LANES), f32),
            pltpu.VMEM((bands, width), f32),
            pltpu.VMEM((bands, width), f32),
            pltpu.VMEM((bands, LANES), f32),
            pltpu.VMEM((bands, LANES), f32),
            pltpu.VMEM((height // LANES, LANES), f32),
            pltpu.VMEM((height // LANES, LANES), f32),
            pltpu.VMEM((2 * BLOCKS + 1, LANES), f32),
            pltpu.VMEM((n_row - 1, 2 * BLOCKS + 1, LANES), f32),
            pltpu.VMEM((bands + BLOCKS, LANES), f32),
            pltpu.VMEM((n_col - 1, bands + BLOCKS, LANES), f32),
            pltpu.SemaphoreType.DMA,
            pltpu.SemaphoreType.DMA,
            pltpu.SemaphoreType.DMA,
            pltpu.SemaphoreType.DMA((n_row - 1,)),
            pltpu.SemaphoreType.DMA,
            pltpu.SemaphoreType.DMA((n_col - 1,)),
            pltpu.SemaphoreType.DMA((bands, blocks)),
            pltpu.SemaphoreType.DMA((len(consts),)),
        ],
        compiler_params=pltpu.CompilerParams(
            collective_id=0, has_side_effects=True, vmem_limit_bytes=59 << 20),
        name="chain",
    )(x, *[jnp.asarray(t) for t in consts])

    return pl.pallas_call(
        finish_kernel,
        out_shape=jax.ShapeDtypeStruct(x.shape, f32),
        in_specs=[vmem, vmem],
        out_specs=hbm,
        scratch_shapes=[
            pltpu.VMEM((height, width), f32),
            pltpu.SemaphoreType.DMA((bands,)),
        ],
        compiler_params=pltpu.CompilerParams(vmem_limit_bytes=16 << 20),
        name="finish",
    )(u, offsets)


def solution(mesh):
    n_row, n_col = mesh.shape["row"], mesh.shape["col"]
    return jax.shard_map(
        functools.partial(per_device, n_row, n_col), mesh=mesh,
        in_specs=(P("row", "col"),), out_specs=P("row", "col"), check_vma=False,
    )
```

```python
import functools
import math

import jax
import jax.numpy as jnp
import numpy as np
from jax import lax
from jax.experimental import pallas as pl
from jax.experimental.pallas import tpu as pltpu
from jax.sharding import PartitionSpec as P

TILE = 256
FULL_TURN = 2.0 * math.pi
MESH = pl.DeviceIdType.MESH
LANES = 128


def wrap_turns(values):
    return values - jnp.round(values)


def cos32(angle):
    return np.cos(angle.astype(np.float64)).astype(np.float32)


def tables(length):
    f32 = np.float32
    order = np.arange(length, dtype=f32)
    angle = (f32(math.pi) * order)[:, None] * (f32(2) * order + f32(1))[None, :] / f32(2 * length)
    cosine = cos32(angle) * f32(math.sqrt(2.0 / length))
    cosine[0] = cosine[0] * f32(math.sqrt(0.5))
    wave = f32(2) * cos32(f32(math.pi) * order / f32(length))
    eigen = (wave[:, None] + wave[None, :]) - f32(4)
    eigen[0, 0] = -1
    inverse = 1.0 / eigen.astype(np.float64)
    inverse[0, 0] = 0
    c64 = cosine.astype(np.float64)
    weights = []
    for cell in (length - 1, 0):
        green = (c64[:, cell] * inverse[0]) @ c64
        step = green - np.append(green[1:], 0.0)
        step[-1] = 0
        weights.append(step / length)
    return cosine, inverse.astype(f32), np.stack(weights).astype(f32)


def split(values):
    high = values.astype(jnp.bfloat16)
    low = (values - high.astype(jnp.float32)).astype(jnp.bfloat16)
    return high, low


def dot(left, right):
    return jnp.dot(left, right, preferred_element_type=jnp.float32)


def stack3(high, low, axis):
    return jnp.concatenate([high, low, high], axis)


BLOCKS = TILE // LANES


def wide(ref, first, rows):
    return jnp.concatenate([ref[first + l, rows, :] for l in range(BLOCKS)], 1)


def put_wide(ref, first, rows, values):
    for l in range(values.shape[1] // LANES):
        ref[first + l, rows, :] = values[:, l * LANES : (l + 1) * LANES]


def in_blocks(table):
    return np.ascontiguousarray(
        table.reshape(table.shape[0], -1, LANES).transpose(1, 0, 2))


def sandwich(pairs, right, left):
    first, second = pl.ds(0, TILE), pl.ds(TILE, TILE)
    table = [wide(right, 0, first), wide(right, 0, first), wide(right, 0, second)]
    table = jnp.concatenate(table, 0)
    inner = [split(dot(stack3(high, low, 1), table)) for high, low in pairs]
    table = [wide(left, 0, first), wide(left, 0, first), wide(left, BLOCKS, first)]
    table = jnp.concatenate(table, 1)
    return [dot(table, stack3(high, low, 0)) for high, low in inner]


def group_size(bands, most):
    return next(g for g in range(most, 0, -1) if bands % g == 0)


def band_rows(i):
    return pl.ds(pl.multiple_of(i * TILE, TILE), TILE)


def band_copy(src, dst, sem, i):
    rows = band_rows(i)
    view = lambda ref: ref.at[rows, :] if len(ref.shape) == 2 else ref.at[:, rows, :]
    return pltpu.make_async_copy(view(src), view(dst), sem.at[i])


def lane_sum(values):
    return jnp.sum(values, axis=1, keepdims=True)


def running(values):
    n = values.shape[0]
    row = lax.broadcasted_iota(jnp.int32, values.shape, 0)
    total = jnp.zeros_like(values)
    for k in range(n - 1):
        total = total + jnp.where(row > k, values[k : k + 1], 0.0)
    return total


def band_sums(values, bands):
    span = TILE // 8
    row = lax.broadcasted_iota(jnp.int32, (bands, LANES), 0)
    lane = lax.broadcasted_iota(jnp.int32, (bands, LANES), 1)
    per = LANES // span
    sums = jnp.sum(values.reshape(-1, 8, LANES), axis=1)
    picked = jnp.concatenate(
        [jnp.broadcast_to(sums[i // per : i // per + 1], (1, LANES)) for i in range(bands)], 0)
    return lane_sum(jnp.where(lane // span == row % per, picked, 0.0))


LOW = 8
STEP = 16
SPAN = 32


def low_tables(length, bands):
    order = np.arange(length, dtype=np.float64)
    exact = np.cos(np.pi * order[:, None] * (2 * order + 1) / (2 * length)) * math.sqrt(2.0 / length)
    exact[0] *= math.sqrt(0.5)
    wave = 2 * np.cos(np.pi * order / length)
    eigen = wave[:, None] + wave[None, :] - 4
    inverse = tables(length)[1].astype(np.float64)
    change = (eigen * inverse - 1)[:LOW, :LOW]
    change[0, 0] = 0
    means = exact[:LOW].reshape(LOW, length // SPAN, SPAN // 8, 8).mean(2).reshape(LOW, -1)
    full = np.zeros((bands * LOW, LANES), np.float32)
    full[:, :LOW] = np.tile(change, (bands, 1))
    return np.kron(np.eye(bands), means).astype(np.float32), full


def slope_band(x_s, wl_ref, wf_ref, step_ref, net_ref, i, d_s, xb_s, cols_s, sum_x, sum_n, sum_l, sum_f):
    blocks = x_s.shape[0]
    base = pl.multiple_of(i * TILE, TILE) + 8
    shape = (STEP, LANES)
    row = lax.broadcasted_iota(jnp.int32, shape, 0)
    lane8 = lax.broadcasted_iota(jnp.int32, (8, LANES), 1)
    bottom, top = row == STEP - 1, row == 0
    f32, bf16 = jnp.float32, jnp.bfloat16
    none = jnp.zeros(shape, bf16)
    zero = jnp.zeros((8, LANES), f32)
    fold = lambda v: v[0:8] + v[8:16]
    counts = lambda v: jnp.round(v * bf16(1.0 / FULL_TURN))
    groups = range(0, TILE, STEP)
    near = [x_s[l, pl.ds(base, TILE), :].astype(bf16) for l in range(blocks)]
    nets, totals = [], []
    for t in range(blocks // BLOCKS):
        some = near[t * BLOCKS : (t + 2) * BLOCKS]
        n = dot(jnp.concatenate(some, 1), step_ref[0 : len(some) * LANES, :])
        n = counts(n.astype(bf16))
        totals.append(functools.reduce(jnp.add, [n[g : g + STEP] for g in groups]))
        nets.append(dot(n, net_ref[...]).astype(bf16))
    acc_x = [zero] * blocks
    acc_l, acc_f = zero, zero
    first, last = zero, zero
    part = [None] * blocks
    halves = [None] * blocks
    for g in groups:
        x = [x_s[l, pl.ds(base + g, STEP), :] for l in range(blocks)]
        tall, whole = [], []
        for l in range(blocks):
            if g == TILE - STEP:
                below = jnp.where(bottom, x[l], pltpu.roll(x[l], STEP - 1, 0))
            else:
                below = x_s[l, pl.ds(base + g + 1, STEP), :]
            above = x_s[l, pl.ds(base + g - 1, STEP), :]
            mine = near[l][g : g + STEP]
            down = counts(below.astype(bf16) - mine)
            up = counts(mine - above.astype(bf16))
            if g == 0:
                up = jnp.where(top, none, up)
            if l < BLOCKS:
                tall.append(below - x[l])
                whole.append(down)
            net = nets[l // BLOCKS][g : g + STEP, l % BLOCKS * LANES : (l % BLOCKS + 1) * LANES]
            d_s[l, pl.ds(base - 8 + g, STEP), :] = net + (down - up)
            half = fold(x[l])
            if g % SPAN == 0:
                part[l] = half
            else:
                total = part[l] + half
                acc_x[l] = acc_x[l] + total
                if g % (2 * SPAN) == STEP:
                    halves[l] = total
                else:
                    xb_s[l, pl.ds(pl.multiple_of(i * (TILE // 4), 16) + g // (2 * SPAN) * 16, 16), :] = (
                        jnp.concatenate([halves[l], total], 0).astype(bf16))
        slope = functools.reduce(jnp.add, tall) * (1.0 / FULL_TURN)
        slope = slope - functools.reduce(jnp.add, whole).astype(f32)
        acc_l = acc_l + fold(slope * wl_ref[g : g + STEP, :])
        acc_f = acc_f + fold(slope * wf_ref[g : g + STEP, :])
        for j in range(STEP // 8):
            k = g // 8 + j
            cells = slice(8 * j, 8 * j + 8)
            first = jnp.where(lane8 == k, pltpu.roll(x[0][cells], k, 1) if k else x[0][cells], first)
            last = jnp.where(lane8 == k, pltpu.roll(x[-1][cells], k + 1, 1), last)
    here = pl.ds(pl.multiple_of(i * 8, 8), 8)
    cols_s[0, here, :] = first
    cols_s[1, here, :] = last
    sum_x[pl.ds(i, 1), :] = jnp.sum(jnp.concatenate(acc_x, 1), axis=0, keepdims=True)
    sum_n[pl.ds(i, 1), :] = jnp.sum(jnp.concatenate(totals, 1).astype(f32), axis=0, keepdims=True)
    sum_l[pl.ds(i, 1), :] = jnp.sum(acc_l, axis=0, keepdims=True)
    sum_f[pl.ds(i, 1), :] = jnp.sum(acc_f, axis=0, keepdims=True)


def gather_cols(cols_s, side, bands):
    span = TILE // 8
    per = LANES // span
    rows = []
    for g in range(0, bands, per):
        parts = [cols_s[side, (g + j) * 8 : (g + j + 1) * 8, :] for j in range(per)]
        parts = [pltpu.roll(v, j * span, 1) if j else v for j, v in enumerate(parts)]
        rows.append(functools.reduce(jnp.add, parts))
    return jnp.concatenate(rows, 0)


def chain_kernel(
    n_row, n_col, x_hbm, step_hbm, net_hbm, wl_hbm, wf_hbm, w_hbm, left_hbm, right_hbm, left_t_hbm, right_t_hbm, inv_hbm,
    low_hbm, change_hbm, u_ref, off_ref,
    x_s, step_ref, net_ref, wl_ref, wf_ref, w_ref, left, right, left_t, right_t, inv_ref, low_ref, change_ref,
    d_s, xb_s, cols_s, corr_s, sum_x, sum_n, sum_l, sum_f,
    col_out, col_in, down_out, down_in, row_out, row_in,
    edge_send, edge_recv, down_send, down_recv, row_send, row_recv,
    x_sem, table_sem,
):
    r, c = lax.axis_index("row"), lax.axis_index("col")
    blocks, height = x_s.shape[0], x_s.shape[1] - 16
    bands, tiles = height // TILE, blocks // BLOCKS

    def x_copy(i, l):
        return pltpu.make_async_copy(
            x_hbm.at[band_rows(i), l * LANES : (l + 1) * LANES], x_s.at[l, pl.ds(pl.multiple_of(i * TILE, TILE) + 8, TILE), :],
            x_sem.at[i, l])

    def fetch(i, carry):
        for l in range(blocks):
            x_copy(i, l).start()
        return carry

    def arrive(i):
        for l in range(blocks):
            x_copy(i, l).wait()

    copies = [(step_hbm, step_ref), (net_hbm, net_ref), (wl_hbm, wl_ref), (wf_hbm, wf_ref), (w_hbm, w_ref), (right_hbm, right), (left_hbm, left),
              (inv_hbm, inv_ref), (low_hbm, low_ref), (change_hbm, change_ref),
              (right_t_hbm, right_t), (left_t_hbm, left_t)]
    copies = [pltpu.make_async_copy(a, b, table_sem.at[k]) for k, (a, b) in enumerate(copies)]
    fetch(0, 0)
    for copy in copies[:4]:
        copy.start()
    lax.fori_loop(1, bands, fetch, 0)
    for copy in copies[4:]:
        copy.start()

    barrier = pltpu.get_barrier_semaphore()

    def greet(row, col):
        pl.semaphore_signal(barrier, inc=1, device_id=(row, col), device_id_type=MESH)

    def greet_above(k, carry):
        greet(k, 0)
        return carry

    def greet_left(k, carry):
        greet(r, k)
        return carry

    is_first = c == 0
    has_right = c < n_col - 1
    lax.fori_loop(0, r, greet_above, 0)
    lax.fori_loop(0, c, greet_left, 0)
    pl.when(has_right)(lambda: greet(r, c + 1))

    pair = group_size(bands, 2)

    def slopes(j, carry):
        for k in range(pair):
            arrive(j * pair + k)
        for k in range(pair):
            slope_band(x_s, wl_ref, wf_ref, step_ref, net_ref, j * pair + k,
                       d_s, xb_s, cols_s, sum_x, sum_n, sum_l, sum_f)
        return carry

    for copy in copies[:4]:
        copy.wait()
    lax.fori_loop(0, bands // pair, slopes, 0)
    col_out[...] = gather_cols(cols_s, 0, bands)
    edge_col = pltpu.make_async_remote_copy(
        src_ref=col_out, dst_ref=col_in, send_sem=edge_send, recv_sem=edge_recv,
        device_id=(r, jnp.maximum(c - 1, 0)), device_id_type=MESH)

    @pl.when(jnp.logical_not(is_first))
    def _():
        pl.semaphore_wait(barrier, n_col - c)
        edge_col.start()

    scale = FULL_TURN / TILE
    down_last = lane_sum(sum_l[...])
    down_first = lane_sum(sum_f[...])
    border = jnp.zeros((bands - 1, LANES), jnp.float32)
    for l in range(BLOCKS):
        ends = [x_s[l, i * TILE + 7 : i * TILE + 9, :] for i in range(1, bands)]
        ends = [v[1:2] - v[0:1] for v in ends]
        border = border + wrap_turns(jnp.concatenate(ends, 0) * (1.0 / FULL_TURN))
    border = lane_sum(border) * scale
    zero = jnp.zeros((1, 1), jnp.float32)
    jump = down_last + jnp.concatenate([border - down_first[1:bands], zero], 0)
    jump_total = jnp.sum(jump, axis=0, keepdims=True) - down_first[0:1]
    starts = running(jump)
    starts = starts - jnp.where(r > 0, down_first[0:1], 0.0)
    lane = lax.broadcasted_iota(jnp.int32, (1, LANES), 1)
    tops = [x_s[l, 8:9, :] for l in range(BLOCKS)]
    scalars = jnp.where(lane == 0, jump_total, jnp.where(lane == 1, down_first[0:1], 0.0))
    down_out[...] = jnp.concatenate(
        tops + [x_s[l, height + 7 : height + 8, :] for l in range(BLOCKS)] + [scalars], 0)

    down_copy = lambda row, col: pltpu.make_async_remote_copy(
        src_ref=down_out, dst_ref=down_in.at[r], send_sem=down_send, recv_sem=down_recv.at[r],
        device_id=(row, col), device_id_type=MESH)
    row_copy = lambda k: pltpu.make_async_remote_copy(
        src_ref=row_out, dst_ref=row_in.at[c], send_sem=row_send, recv_sem=row_recv.at[c],
        device_id=(r, k), device_id_type=MESH)
    for copy in copies[4:]:
        copy.wait()
    first, second = pl.ds(0, TILE), pl.ds(TILE, TILE)
    for t in range(tiles):
        low = jnp.concatenate([xb_s[t * BLOCKS + k] for k in range(BLOCKS)], 1)
        low = dot(low, right[0, first, :]).astype(jnp.bfloat16)
        corr_s[t] = dot(low_ref[...], low) * change_ref[...]

    def solve(some):
        places = [(i, t) for i in some for t in range(tiles)]
        table = jnp.concatenate([wide(right, 0, first), wide(right, 0, second)], 0)
        data = [wide(d_s, t * BLOCKS, band_rows(i)) for i, t in places]
        inner = [split(dot(jnp.concatenate([d, d], 1), table)) for d in data]
        table = [wide(left, 0, first), wide(left, 0, first), wide(left, BLOCKS, first)]
        table = jnp.concatenate(table, 1)
        pairs = []
        for (i, t), (high, low) in zip(places, inner):
            scaled = dot(table, stack3(high, low, 0)) * inv_ref[...]
            corner = scaled[0:LOW, 0:LANES] + corr_s[t, i * LOW : (i + 1) * LOW, :]
            scaled = jnp.concatenate(
                [jnp.concatenate([corner, scaled[0:LOW, LANES:]], 1), scaled[LOW:]], 0)
            pairs.append(split(scaled))
        for (i, t), solved in zip(places, sandwich(pairs, right_t, left_t)):
            u_ref[band_rows(i), t * TILE : (t + 1) * TILE] = (
                solved + wide(x_s, t * BLOCKS, pl.ds(i * TILE + 8, TILE)))

    solve(range(0, 2))

    def each_below(act):
        def per_row(k, carry):
            def per_col(j, carry):
                act(down_copy(n_row - 1 - k, n_col - 1 - j))
                return carry
            return lax.fori_loop(0, n_col, per_col, carry)
        lax.fori_loop(0, jnp.where(is_first, n_row - 1 - r, 0), per_row, 0)

    def send_down(when):
        @pl.when(jnp.logical_and(is_first, when))
        def _():
            pl.semaphore_wait(barrier, (n_row - 1 - r) * n_col + n_col - 1)
            each_below(lambda copy: copy.start())

    send_down(r > 0)
    solve(range(2, 4))
    send_down(r == 0)

    last_col = gather_cols(cols_s, 1, bands)
    sums = sum_x[...]
    mean = [lane_sum(sums[:, t * TILE : (t + 1) * TILE]) * (1.0 / TILE / TILE) for t in range(tiles)]
    sums = (pltpu.roll(sums, blocks * LANES - 1, 1) - sums) * (1.0 / FULL_TURN) - sum_n[...]
    last_w, first_w = w_ref[0:1, 0:TILE], w_ref[0:1, TILE : 2 * TILE]
    lasts = [lane_sum(sums[:, t * TILE : (t + 1) * TILE] * last_w) for t in range(tiles)]
    firsts = [lane_sum(sums[:, t * TILE : (t + 1) * TILE] * first_w) for t in range(tiles)]
    along = [jnp.zeros((bands, 1), jnp.float32)]
    for t in range(tiles - 1):
        end = (t + 1) * TILE
        along.append(along[-1] + lasts[t] + sums[:, end - 1 : end] * scale - firsts[t + 1])

    pl.when(has_right)(lambda: edge_col.wait_recv())
    edge = wrap_turns((col_in[...] - last_col) * (1.0 / FULL_TURN))
    row_total = along[-1] + lasts[-1] + band_sums(edge, bands) * scale - firsts[0]
    lane = lax.broadcasted_iota(jnp.int32, (bands, LANES), 1)
    row_out[0:bands, :] = jnp.where(
        lane == 0, row_total, jnp.where(lane == 1, starts + firsts[0], 0.0))
    row_out[bands : bands + BLOCKS, :] = jnp.concatenate(tops, 0)

    def send_row(k, carry):
        row_copy(k).start()
        return carry

    lax.fori_loop(c + 1, n_col, send_row, 0)

    for k in range(4, bands, 4):
        solve(range(k, min(k + 4, bands)))

    pl.when(jnp.logical_not(is_first))(lambda: edge_col.wait_send())

    each_below(lambda copy: copy.wait_send())

    def sent_row(k, carry):
        row_copy(k).wait_send()
        return carry

    lax.fori_loop(c + 1, n_col, sent_row, 0)

    offset = jnp.where(is_first, starts, -firsts[0])
    for k in range(n_col - 1):
        pl.when(k < c)(lambda: pltpu.make_async_remote_copy(
            src_ref=row_out, dst_ref=row_in.at[k], send_sem=row_send, recv_sem=row_recv.at[k],
            device_id=(r, c), device_id_type=MESH).wait_recv())
        offset = offset + jnp.where(k < c, row_in[k, 0:bands, 0:1], 0.0)
    offset = offset + jnp.where(c > 0, row_in[0, 0:bands, 1:2], 0.0)

    for k in range(n_row - 1):
        pl.when(k < r)(lambda: pltpu.make_async_remote_copy(
            src_ref=down_out, dst_ref=down_in.at[k], send_sem=down_send, recv_sem=down_recv.at[k],
            device_id=(r, c), device_id_type=MESH).wait_recv())
    edge = jnp.zeros((n_row - 1, LANES), jnp.float32)
    number = lax.broadcasted_iota(jnp.int32, (n_row - 1, LANES), 0)
    for l in range(BLOCKS):
        own = jnp.where(is_first, tops[l], row_in[0, bands + l : bands + l + 1, :])
        upper = jnp.concatenate([down_in[k, BLOCKS + l : BLOCKS + l + 1, :] for k in range(n_row - 1)], 0)
        lower = jnp.concatenate([down_in[k, l : l + 1, :] for k in range(1, n_row - 1)] + [own], 0)
        lower = jnp.where(number == r - 1, own, lower)
        edge = edge + wrap_turns((lower - upper) * (1.0 / FULL_TURN))
    single = jnp.concatenate([down_in[k, 2 * BLOCKS : 2 * BLOCKS + 1, :] for k in range(n_row - 1)], 0)
    lane = lax.broadcasted_iota(jnp.int32, (n_row - 1, LANES), 1)
    pick = jnp.where(lane == 0, single, 0.0) + jnp.where((lane == 1) & (number == 0), single, 0.0)
    above = jnp.where(number < r, edge * scale + pick, 0.0)
    above = lane_sum(jnp.sum(above, axis=0, keepdims=True))
    offset = offset + above
    for t in range(tiles):
        off_ref[:, t * TILE : (t + 1) * TILE] = jnp.broadcast_to(
            offset + along[t] - mean[t], (bands, TILE))


def finish_kernel(u_ref, off_ref, out_hbm, out_s, out_sem):
    height, width = out_s.shape
    bands = height // TILE
    for i in range(bands):
        rows = band_rows(i)
        out_s[rows, :] = u_ref[rows, :] + off_ref[i : i + 1, :]
        band_copy(out_s, out_hbm, out_sem, i).start()
    for i in range(bands):
        band_copy(out_s, out_hbm, out_sem, i).wait()


def per_device(n_row, n_col, x):
    height, width = x.shape
    bands = height // TILE
    blocks = width // LANES
    tiles = width // TILE
    cosine, inverse, weights = tables(TILE)
    high = cosine.astype(jnp.bfloat16)
    low = (cosine - high.astype(np.float32)).astype(jnp.bfloat16)
    beside = in_blocks(np.concatenate([high, low], 1))
    over = in_blocks(np.concatenate([high, low], 0))
    beside_t = in_blocks(np.concatenate([high.T, low.T], 1))
    over_t = in_blocks(np.concatenate([high.T, low.T], 0))
    weights = weights * np.float32(FULL_TURN)
    w = np.tile(weights.reshape(1, -1), (8, 1))
    wl = np.ascontiguousarray(np.broadcast_to(weights[0][:, None], (TILE, LANES)))
    wf = np.ascontiguousarray(np.broadcast_to(weights[1][:, None], (TILE, LANES)))
    means, change = low_tables(TILE, bands)
    eye = np.eye(2 * TILE, TILE, dtype=np.float32)
    step = np.eye(2 * TILE, TILE, -1, dtype=np.float32) - eye
    net = np.eye(TILE, dtype=np.float32) - np.eye(TILE, k=1, dtype=np.float32)
    net[TILE - 1] = 0

    vmem = pl.BlockSpec(memory_space=pltpu.VMEM)
    hbm = pl.BlockSpec(memory_space=pltpu.HBM)
    f32, bf16 = jnp.float32, jnp.bfloat16
    consts = [step.astype(bf16), net.astype(bf16), wl, wf, w, beside, over_t, beside_t, over, inverse * np.float32(-FULL_TURN),
              means.astype(bf16), change]
    u, offsets = pl.pallas_call(
        functools.partial(chain_kernel, n_row, n_col),
        out_shape=[pltpu.VMEM(x.shape, f32), pltpu.VMEM((bands, width), f32)],
        in_specs=[hbm] * (1 + len(consts)),
        out_specs=[vmem, vmem],
        scratch_shapes=[pltpu.VMEM((blocks, height + 16, LANES), f32)]
        + [pltpu.VMEM(t.shape, t.dtype) for t in consts]
        + [
            pltpu.VMEM((blocks, height, LANES), bf16),
            pltpu.VMEM((blocks, height // 4, LANES), bf16),
            pltpu.VMEM((2, bands * 8, LANES), f32),
            pltpu.VMEM((tiles, bands * LOW, LANES), f32),
            pltpu.VMEM((bands, width), f32),
            pltpu.VMEM((bands, width), f32),
            pltpu.VMEM((bands, LANES), f32),
            pltpu.VMEM((bands, LANES), f32),
            pltpu.VMEM((height // LANES, LANES), f32),
            pltpu.VMEM((height // LANES, LANES), f32),
            pltpu.VMEM((2 * BLOCKS + 1, LANES), f32),
            pltpu.VMEM((n_row - 1, 2 * BLOCKS + 1, LANES), f32),
            pltpu.VMEM((bands + BLOCKS, LANES), f32),
            pltpu.VMEM((n_col - 1, bands + BLOCKS, LANES), f32),
            pltpu.SemaphoreType.DMA,
            pltpu.SemaphoreType.DMA,
            pltpu.SemaphoreType.DMA,
            pltpu.SemaphoreType.DMA((n_row - 1,)),
            pltpu.SemaphoreType.DMA,
            pltpu.SemaphoreType.DMA((n_col - 1,)),
            pltpu.SemaphoreType.DMA((bands, blocks)),
            pltpu.SemaphoreType.DMA((len(consts),)),
        ],
        compiler_params=pltpu.CompilerParams(
            collective_id=0, has_side_effects=True, vmem_limit_bytes=59 << 20),
        name="chain",
    )(x, *[jnp.asarray(t) for t in consts])

    return pl.pallas_call(
        finish_kernel,
        out_shape=jax.ShapeDtypeStruct(x.shape, f32),
        in_specs=[vmem, vmem],
        out_specs=hbm,
        scratch_shapes=[
            pltpu.VMEM((height, width), f32),
            pltpu.SemaphoreType.DMA((bands,)),
        ],
        compiler_params=pltpu.CompilerParams(vmem_limit_bytes=16 << 20),
        name="finish",
    )(u, offsets)


def solution(mesh):
    n_row, n_col = mesh.shape["row"], mesh.shape["col"]
    return jax.shard_map(
        functools.partial(per_device, n_row, n_col), mesh=mesh,
        in_specs=(P("row", "col"),), out_specs=P("row", "col"), check_vma=False,
    )
```

```python
import functools
import math

import jax
import jax.numpy as jnp
import numpy as np
from jax import lax
from jax.experimental import pallas as pl
from jax.experimental.pallas import tpu as pltpu
from jax.sharding import PartitionSpec as P

TILE = 256
FULL_TURN = 2.0 * math.pi
MESH = pl.DeviceIdType.MESH
LANES = 128


def wrap_turns(values):
    return values - jnp.round(values)


def cos32(angle):
    return np.cos(angle.astype(np.float64)).astype(np.float32)


def tables(length):
    f32 = np.float32
    order = np.arange(length, dtype=f32)
    angle = (f32(math.pi) * order)[:, None] * (f32(2) * order + f32(1))[None, :] / f32(2 * length)
    cosine = cos32(angle) * f32(math.sqrt(2.0 / length))
    cosine[0] = cosine[0] * f32(math.sqrt(0.5))
    wave = f32(2) * cos32(f32(math.pi) * order / f32(length))
    eigen = (wave[:, None] + wave[None, :]) - f32(4)
    eigen[0, 0] = -1
    inverse = 1.0 / eigen.astype(np.float64)
    inverse[0, 0] = 0
    c64 = cosine.astype(np.float64)
    weights = []
    for cell in (length - 1, 0):
        green = (c64[:, cell] * inverse[0]) @ c64
        step = green - np.append(green[1:], 0.0)
        step[-1] = 0
        weights.append(step / length)
    return cosine, inverse.astype(f32), np.stack(weights).astype(f32)


def split(values):
    high = values.astype(jnp.bfloat16)
    low = (values - high.astype(jnp.float32)).astype(jnp.bfloat16)
    return high, low


def dot(left, right):
    return jnp.dot(left, right, preferred_element_type=jnp.float32)


def stack3(high, low, axis):
    return jnp.concatenate([high, low, high], axis)


BLOCKS = TILE // LANES


def wide(ref, first, rows):
    return jnp.concatenate([ref[first + l, rows, :] for l in range(BLOCKS)], 1)


def put_wide(ref, first, rows, values):
    for l in range(values.shape[1] // LANES):
        ref[first + l, rows, :] = values[:, l * LANES : (l + 1) * LANES]


def in_blocks(table):
    return np.ascontiguousarray(
        table.reshape(table.shape[0], -1, LANES).transpose(1, 0, 2))


def sandwich(pairs, right, left):
    first, second = pl.ds(0, TILE), pl.ds(TILE, TILE)
    table = [wide(right, 0, first), wide(right, 0, first), wide(right, 0, second)]
    table = jnp.concatenate(table, 0)
    inner = [split(dot(stack3(high, low, 1), table)) for high, low in pairs]
    table = [wide(left, 0, first), wide(left, 0, first), wide(left, BLOCKS, first)]
    table = jnp.concatenate(table, 1)
    return [dot(table, stack3(high, low, 0)) for high, low in inner]


def group_size(bands, most):
    return next(g for g in range(most, 0, -1) if bands % g == 0)


def band_rows(i):
    return pl.ds(pl.multiple_of(i * TILE, TILE), TILE)


def band_copy(src, dst, sem, i):
    rows = band_rows(i)
    view = lambda ref: ref.at[rows, :] if len(ref.shape) == 2 else ref.at[:, rows, :]
    return pltpu.make_async_copy(view(src), view(dst), sem.at[i])


def lane_sum(values):
    return jnp.sum(values, axis=1, keepdims=True)


def running(values):
    n = values.shape[0]
    row = lax.broadcasted_iota(jnp.int32, values.shape, 0)
    total = jnp.zeros_like(values)
    for k in range(n - 1):
        total = total + jnp.where(row > k, values[k : k + 1], 0.0)
    return total


def band_sums(values, bands):
    span = TILE // 8
    row = lax.broadcasted_iota(jnp.int32, (bands, LANES), 0)
    lane = lax.broadcasted_iota(jnp.int32, (bands, LANES), 1)
    per = LANES // span
    sums = jnp.sum(values.reshape(-1, 8, LANES), axis=1)
    picked = jnp.concatenate(
        [jnp.broadcast_to(sums[i // per : i // per + 1], (1, LANES)) for i in range(bands)], 0)
    return lane_sum(jnp.where(lane // span == row % per, picked, 0.0))


LOW = 8
STEP = 16
SPAN = 32


def low_tables(length, bands):
    order = np.arange(length, dtype=np.float64)
    exact = np.cos(np.pi * order[:, None] * (2 * order + 1) / (2 * length)) * math.sqrt(2.0 / length)
    exact[0] *= math.sqrt(0.5)
    wave = 2 * np.cos(np.pi * order / length)
    eigen = wave[:, None] + wave[None, :] - 4
    inverse = tables(length)[1].astype(np.float64)
    change = (eigen * inverse - 1)[:LOW, :LOW]
    change[0, 0] = 0
    means = exact[:LOW].reshape(LOW, length // SPAN, SPAN // 8, 8).mean(2).reshape(LOW, -1)
    full = np.zeros((bands * LOW, LANES), np.float32)
    full[:, :LOW] = np.tile(change, (bands, 1))
    return np.kron(np.eye(bands), means).astype(np.float32), full


def slope_band(x_s, wl_ref, wf_ref, step_ref, net_ref, i, d_s, xb_s, cols_s, sum_x, sum_n, sum_l, sum_f):
    blocks = x_s.shape[0]
    base = pl.multiple_of(i * TILE, TILE) + 8
    shape = (STEP, LANES)
    row = lax.broadcasted_iota(jnp.int32, shape, 0)
    lane8 = lax.broadcasted_iota(jnp.int32, (8, LANES), 1)
    bottom, top = row == STEP - 1, row == 0
    f32, bf16 = jnp.float32, jnp.bfloat16
    none = jnp.zeros(shape, bf16)
    zero = jnp.zeros((8, LANES), f32)
    fold = lambda v: v[0:8] + v[8:16]
    counts = lambda v: jnp.round(v * bf16(1.0 / FULL_TURN))
    groups = range(0, TILE, STEP)
    near_of = lambda l, g, size: x_s[l, pl.ds(base + g, size), :].astype(bf16)
    totals = []
    acc_x = [zero] * blocks
    acc_l, acc_f = zero, zero
    first, last = zero, zero
    for t in range(blocks // BLOCKS):
        own = range(t * BLOCKS, (t + 1) * BLOCKS)
        some = range(t * BLOCKS, min((t + 2) * BLOCKS, blocks))
        n = dot(jnp.concatenate([near_of(l, 0, TILE) for l in some], 1),
                step_ref[0 : len(some) * LANES, :])
        n = counts(n.astype(bf16))
        totals.append(functools.reduce(jnp.add, [n[g : g + STEP] for g in groups]))
        nets = dot(n, net_ref[...]).astype(bf16)
        part, halves = {}, {}
        for g in groups:
            tall, whole = [], []
            for l in own:
                x = x_s[l, pl.ds(base + g, STEP), :]
                mine = x.astype(bf16)
                if g == TILE - STEP:
                    below = jnp.where(bottom, x, pltpu.roll(x, STEP - 1, 0))
                else:
                    below = x_s[l, pl.ds(base + g + 1, STEP), :]
                above = x_s[l, pl.ds(base + g - 1, STEP), :]
                down = counts(below.astype(bf16) - mine)
                up = counts(mine - above.astype(bf16))
                if g == 0:
                    up = jnp.where(top, none, up)
                if t == 0:
                    tall.append(below - x)
                    whole.append(down)
                net = nets[g : g + STEP, l % BLOCKS * LANES : (l % BLOCKS + 1) * LANES]
                d_s[l, pl.ds(base - 8 + g, STEP), :] = net + (down - up)
                half = fold(x)
                if g % SPAN == 0:
                    part[l] = half
                else:
                    total = part[l] + half
                    acc_x[l] = acc_x[l] + total
                    if g % (2 * SPAN) == STEP:
                        halves[l] = total
                    else:
                        xb_s[l, pl.ds(pl.multiple_of(i * (TILE // 4), 16) + g // (2 * SPAN) * 16, 16), :] = (
                            jnp.concatenate([halves[l], total], 0).astype(bf16))
                for j in range(STEP // 8):
                    k = g // 8 + j
                    cells = x[8 * j : 8 * j + 8]
                    if l == 0:
                        first = jnp.where(lane8 == k, pltpu.roll(cells, k, 1) if k else cells, first)
                    if l == blocks - 1:
                        last = jnp.where(lane8 == k, pltpu.roll(cells, k + 1, 1), last)
            if t == 0:
                slope = functools.reduce(jnp.add, tall) * (1.0 / FULL_TURN)
                slope = slope - functools.reduce(jnp.add, whole).astype(f32)
                acc_l = acc_l + fold(slope * wl_ref[g : g + STEP, :])
                acc_f = acc_f + fold(slope * wf_ref[g : g + STEP, :])
    here = pl.ds(pl.multiple_of(i * 8, 8), 8)
    cols_s[0, here, :] = first
    cols_s[1, here, :] = last
    sum_x[pl.ds(i, 1), :] = jnp.sum(jnp.concatenate(acc_x, 1), axis=0, keepdims=True)
    sum_n[pl.ds(i, 1), :] = jnp.sum(jnp.concatenate(totals, 1).astype(f32), axis=0, keepdims=True)
    sum_l[pl.ds(i, 1), :] = jnp.sum(acc_l, axis=0, keepdims=True)
    sum_f[pl.ds(i, 1), :] = jnp.sum(acc_f, axis=0, keepdims=True)


def gather_cols(cols_s, side, bands):
    span = TILE // 8
    per = LANES // span
    rows = []
    for g in range(0, bands, per):
        parts = [cols_s[side, (g + j) * 8 : (g + j + 1) * 8, :] for j in range(per)]
        parts = [pltpu.roll(v, j * span, 1) if j else v for j, v in enumerate(parts)]
        rows.append(functools.reduce(jnp.add, parts))
    return jnp.concatenate(rows, 0)


def chain_kernel(
    n_row, n_col, x_hbm, step_hbm, net_hbm, wl_hbm, wf_hbm, w_hbm, left_hbm, right_hbm, left_t_hbm, right_t_hbm, inv_hbm,
    low_hbm, change_hbm, u_ref, off_ref,
    x_s, step_ref, net_ref, wl_ref, wf_ref, w_ref, left, right, left_t, right_t, inv_ref, low_ref, change_ref,
    d_s, xb_s, cols_s, corr_s, sum_x, sum_n, sum_l, sum_f,
    col_out, col_in, down_out, down_in, row_out, row_in,
    edge_send, edge_recv, down_send, down_recv, row_send, row_recv,
    x_sem, table_sem,
):
    r, c = lax.axis_index("row"), lax.axis_index("col")
    blocks, height = x_s.shape[0], x_s.shape[1] - 16
    bands, tiles = height // TILE, blocks // BLOCKS

    def x_copy(i, l):
        return pltpu.make_async_copy(
            x_hbm.at[band_rows(i), l * LANES : (l + 1) * LANES], x_s.at[l, pl.ds(pl.multiple_of(i * TILE, TILE) + 8, TILE), :],
            x_sem.at[i, l])

    def fetch(i, carry):
        for l in range(blocks):
            x_copy(i, l).start()
        return carry

    def arrive(i):
        for l in range(blocks):
            x_copy(i, l).wait()

    copies = [(step_hbm, step_ref), (net_hbm, net_ref), (wl_hbm, wl_ref), (wf_hbm, wf_ref), (w_hbm, w_ref), (right_hbm, right), (left_hbm, left),
              (inv_hbm, inv_ref), (low_hbm, low_ref), (change_hbm, change_ref),
              (right_t_hbm, right_t), (left_t_hbm, left_t)]
    copies = [pltpu.make_async_copy(a, b, table_sem.at[k]) for k, (a, b) in enumerate(copies)]
    fetch(0, 0)
    for copy in copies[:4]:
        copy.start()
    lax.fori_loop(1, bands, fetch, 0)
    for copy in copies[4:]:
        copy.start()

    barrier = pltpu.get_barrier_semaphore()

    def greet(row, col):
        pl.semaphore_signal(barrier, inc=1, device_id=(row, col), device_id_type=MESH)

    def greet_above(k, carry):
        greet(k, 0)
        return carry

    def greet_left(k, carry):
        greet(r, k)
        return carry

    is_first = c == 0
    has_right = c < n_col - 1
    lax.fori_loop(0, r, greet_above, 0)
    lax.fori_loop(0, c, greet_left, 0)
    pl.when(has_right)(lambda: greet(r, c + 1))

    pair = group_size(bands, 4)

    def slopes(j, carry):
        for k in range(pair):
            arrive(j * pair + k)
        for k in range(pair):
            slope_band(x_s, wl_ref, wf_ref, step_ref, net_ref, j * pair + k,
                       d_s, xb_s, cols_s, sum_x, sum_n, sum_l, sum_f)
        return carry

    for copy in copies[:4]:
        copy.wait()
    lax.fori_loop(0, bands // pair, slopes, 0)
    col_out[...] = gather_cols(cols_s, 0, bands)
    edge_col = pltpu.make_async_remote_copy(
        src_ref=col_out, dst_ref=col_in, send_sem=edge_send, recv_sem=edge_recv,
        device_id=(r, jnp.maximum(c - 1, 0)), device_id_type=MESH)

    @pl.when(jnp.logical_not(is_first))
    def _():
        pl.semaphore_wait(barrier, n_col - c)
        edge_col.start()

    scale = FULL_TURN / TILE
    down_last = lane_sum(sum_l[...])
    down_first = lane_sum(sum_f[...])
    border = jnp.zeros((bands - 1, LANES), jnp.float32)
    for l in range(BLOCKS):
        ends = [x_s[l, i * TILE + 7 : i * TILE + 9, :] for i in range(1, bands)]
        ends = [v[1:2] - v[0:1] for v in ends]
        border = border + wrap_turns(jnp.concatenate(ends, 0) * (1.0 / FULL_TURN))
    border = lane_sum(border) * scale
    zero = jnp.zeros((1, 1), jnp.float32)
    jump = down_last + jnp.concatenate([border - down_first[1:bands], zero], 0)
    jump_total = jnp.sum(jump, axis=0, keepdims=True) - down_first[0:1]
    starts = running(jump)
    starts = starts - jnp.where(r > 0, down_first[0:1], 0.0)
    lane = lax.broadcasted_iota(jnp.int32, (1, LANES), 1)
    tops = [x_s[l, 8:9, :] for l in range(BLOCKS)]
    scalars = jnp.where(lane == 0, jump_total, jnp.where(lane == 1, down_first[0:1], 0.0))
    down_out[...] = jnp.concatenate(
        tops + [x_s[l, height + 7 : height + 8, :] for l in range(BLOCKS)] + [scalars], 0)

    down_copy = lambda row, col: pltpu.make_async_remote_copy(
        src_ref=down_out, dst_ref=down_in.at[r], send_sem=down_send, recv_sem=down_recv.at[r],
        device_id=(row, col), device_id_type=MESH)
    row_copy = lambda k: pltpu.make_async_remote_copy(
        src_ref=row_out, dst_ref=row_in.at[c], send_sem=row_send, recv_sem=row_recv.at[c],
        device_id=(r, k), device_id_type=MESH)
    for copy in copies[4:]:
        copy.wait()
    first, second = pl.ds(0, TILE), pl.ds(TILE, TILE)
    for t in range(tiles):
        low = jnp.concatenate([xb_s[t * BLOCKS + k] for k in range(BLOCKS)], 1)
        low = dot(low, right[0, first, :]).astype(jnp.bfloat16)
        corr_s[t] = dot(low_ref[...], low) * change_ref[...]

    def solve(some):
        places = [(i, t) for i in some for t in range(tiles)]
        table = jnp.concatenate([wide(right, 0, first), wide(right, 0, second)], 0)
        data = [wide(d_s, t * BLOCKS, band_rows(i)) for i, t in places]
        inner = [split(dot(jnp.concatenate([d, d], 1), table)) for d in data]
        table = [wide(left, 0, first), wide(left, 0, first), wide(left, BLOCKS, first)]
        table = jnp.concatenate(table, 1)
        pairs = []
        for (i, t), (high, low) in zip(places, inner):
            scaled = dot(table, stack3(high, low, 0)) * inv_ref[...]
            corner = scaled[0:LOW, 0:LANES] + corr_s[t, i * LOW : (i + 1) * LOW, :]
            scaled = jnp.concatenate(
                [jnp.concatenate([corner, scaled[0:LOW, LANES:]], 1), scaled[LOW:]], 0)
            pairs.append(split(scaled))
        for (i, t), solved in zip(places, sandwich(pairs, right_t, left_t)):
            u_ref[band_rows(i), t * TILE : (t + 1) * TILE] = (
                solved + wide(x_s, t * BLOCKS, pl.ds(i * TILE + 8, TILE)))

    solve(range(0, 2))

    def each_below(act):
        def per_row(k, carry):
            def per_col(j, carry):
                act(down_copy(n_row - 1 - k, n_col - 1 - j))
                return carry
            return lax.fori_loop(0, n_col, per_col, carry)
        lax.fori_loop(0, jnp.where(is_first, n_row - 1 - r, 0), per_row, 0)

    def send_down(when):
        @pl.when(jnp.logical_and(is_first, when))
        def _():
            pl.semaphore_wait(barrier, (n_row - 1 - r) * n_col + n_col - 1)
            each_below(lambda copy: copy.start())

    send_down(r > 0)
    solve(range(2, 4))
    send_down(r == 0)

    last_col = gather_cols(cols_s, 1, bands)
    sums = sum_x[...]
    mean = [lane_sum(sums[:, t * TILE : (t + 1) * TILE]) * (1.0 / TILE / TILE) for t in range(tiles)]
    sums = (pltpu.roll(sums, blocks * LANES - 1, 1) - sums) * (1.0 / FULL_TURN) - sum_n[...]
    last_w, first_w = w_ref[0:1, 0:TILE], w_ref[0:1, TILE : 2 * TILE]
    lasts = [lane_sum(sums[:, t * TILE : (t + 1) * TILE] * last_w) for t in range(tiles)]
    firsts = [lane_sum(sums[:, t * TILE : (t + 1) * TILE] * first_w) for t in range(tiles)]
    along = [jnp.zeros((bands, 1), jnp.float32)]
    for t in range(tiles - 1):
        end = (t + 1) * TILE
        along.append(along[-1] + lasts[t] + sums[:, end - 1 : end] * scale - firsts[t + 1])

    pl.when(has_right)(lambda: edge_col.wait_recv())
    edge = wrap_turns((col_in[...] - last_col) * (1.0 / FULL_TURN))
    row_total = along[-1] + lasts[-1] + band_sums(edge, bands) * scale - firsts[0]
    lane = lax.broadcasted_iota(jnp.int32, (bands, LANES), 1)
    row_out[0:bands, :] = jnp.where(
        lane == 0, row_total, jnp.where(lane == 1, starts + firsts[0], 0.0))
    row_out[bands : bands + BLOCKS, :] = jnp.concatenate(tops, 0)

    def send_row(k, carry):
        row_copy(k).start()
        return carry

    lax.fori_loop(c + 1, n_col, send_row, 0)

    for k in range(4, bands, 4):
        solve(range(k, min(k + 4, bands)))

    pl.when(jnp.logical_not(is_first))(lambda: edge_col.wait_send())

    def sent_below(k, carry):
        some = down_in.at[0:n_col]
        pltpu.make_async_remote_copy(
            src_ref=some, dst_ref=some, send_sem=down_send, recv_sem=down_recv.at[0],
            device_id=(r, c), device_id_type=MESH).wait_send()
        return carry

    lax.fori_loop(0, jnp.where(is_first, n_row - 1 - r, 0), sent_below, 0)

    def sent_row(k, carry):
        row_copy(k).wait_send()
        return carry

    lax.fori_loop(c + 1, n_col, sent_row, 0)

    offset = jnp.where(is_first, starts, -firsts[0])
    for k in range(n_col - 1):
        pl.when(k < c)(lambda: pltpu.make_async_remote_copy(
            src_ref=row_out, dst_ref=row_in.at[k], send_sem=row_send, recv_sem=row_recv.at[k],
            device_id=(r, c), device_id_type=MESH).wait_recv())
        offset = offset + jnp.where(k < c, row_in[k, 0:bands, 0:1], 0.0)
    offset = offset + jnp.where(c > 0, row_in[0, 0:bands, 1:2], 0.0)

    for k in range(n_row - 1):
        pl.when(k < r)(lambda: pltpu.make_async_remote_copy(
            src_ref=down_out, dst_ref=down_in.at[k], send_sem=down_send, recv_sem=down_recv.at[k],
            device_id=(r, c), device_id_type=MESH).wait_recv())
    edge = jnp.zeros((n_row - 1, LANES), jnp.float32)
    number = lax.broadcasted_iota(jnp.int32, (n_row - 1, LANES), 0)
    for l in range(BLOCKS):
        own = jnp.where(is_first, tops[l], row_in[0, bands + l : bands + l + 1, :])
        upper = jnp.concatenate([down_in[k, BLOCKS + l : BLOCKS + l + 1, :] for k in range(n_row - 1)], 0)
        lower = jnp.concatenate([down_in[k, l : l + 1, :] for k in range(1, n_row - 1)] + [own], 0)
        lower = jnp.where(number == r - 1, own, lower)
        edge = edge + wrap_turns((lower - upper) * (1.0 / FULL_TURN))
    single = jnp.concatenate([down_in[k, 2 * BLOCKS : 2 * BLOCKS + 1, :] for k in range(n_row - 1)], 0)
    lane = lax.broadcasted_iota(jnp.int32, (n_row - 1, LANES), 1)
    pick = jnp.where(lane == 0, single, 0.0) + jnp.where((lane == 1) & (number == 0), single, 0.0)
    above = jnp.where(number < r, edge * scale + pick, 0.0)
    above = lane_sum(jnp.sum(above, axis=0, keepdims=True))
    offset = offset + above
    for t in range(tiles):
        off_ref[:, t * TILE : (t + 1) * TILE] = jnp.broadcast_to(
            offset + along[t] - mean[t], (bands, TILE))


def finish_kernel(u_ref, off_ref, out_hbm, out_s, out_sem):
    height, width = out_s.shape
    bands = height // TILE
    for i in range(bands):
        rows = band_rows(i)
        out_s[rows, :] = u_ref[rows, :] + off_ref[i : i + 1, :]
        band_copy(out_s, out_hbm, out_sem, i).start()
    for i in range(bands):
        band_copy(out_s, out_hbm, out_sem, i).wait()


def per_device(n_row, n_col, x):
    height, width = x.shape
    bands = height // TILE
    blocks = width // LANES
    tiles = width // TILE
    cosine, inverse, weights = tables(TILE)
    high = cosine.astype(jnp.bfloat16)
    low = (cosine - high.astype(np.float32)).astype(jnp.bfloat16)
    beside = in_blocks(np.concatenate([high, low], 1))
    over = in_blocks(np.concatenate([high, low], 0))
    beside_t = in_blocks(np.concatenate([high.T, low.T], 1))
    over_t = in_blocks(np.concatenate([high.T, low.T], 0))
    weights = weights * np.float32(FULL_TURN)
    w = np.tile(weights.reshape(1, -1), (8, 1))
    wl = np.ascontiguousarray(np.broadcast_to(weights[0][:, None], (TILE, LANES)))
    wf = np.ascontiguousarray(np.broadcast_to(weights[1][:, None], (TILE, LANES)))
    means, change = low_tables(TILE, bands)
    eye = np.eye(2 * TILE, TILE, dtype=np.float32)
    step = np.eye(2 * TILE, TILE, -1, dtype=np.float32) - eye
    net = np.eye(TILE, dtype=np.float32) - np.eye(TILE, k=1, dtype=np.float32)
    net[TILE - 1] = 0

    vmem = pl.BlockSpec(memory_space=pltpu.VMEM)
    hbm = pl.BlockSpec(memory_space=pltpu.HBM)
    f32, bf16 = jnp.float32, jnp.bfloat16
    consts = [step.astype(bf16), net.astype(bf16), wl, wf, w, beside, over_t, beside_t, over, inverse * np.float32(-FULL_TURN),
              means.astype(bf16), change]
    u, offsets = pl.pallas_call(
        functools.partial(chain_kernel, n_row, n_col),
        out_shape=[pltpu.VMEM(x.shape, f32), pltpu.VMEM((bands, width), f32)],
        in_specs=[hbm] * (1 + len(consts)),
        out_specs=[vmem, vmem],
        scratch_shapes=[pltpu.VMEM((blocks, height + 16, LANES), f32)]
        + [pltpu.VMEM(t.shape, t.dtype) for t in consts]
        + [
            pltpu.VMEM((blocks, height, LANES), bf16),
            pltpu.VMEM((blocks, height // 4, LANES), bf16),
            pltpu.VMEM((2, bands * 8, LANES), f32),
            pltpu.VMEM((tiles, bands * LOW, LANES), f32),
            pltpu.VMEM((bands, width), f32),
            pltpu.VMEM((bands, width), f32),
            pltpu.VMEM((bands, LANES), f32),
            pltpu.VMEM((bands, LANES), f32),
            pltpu.VMEM((height // LANES, LANES), f32),
            pltpu.VMEM((height // LANES, LANES), f32),
            pltpu.VMEM((2 * BLOCKS + 1, LANES), f32),
            pltpu.VMEM((n_row - 1, 2 * BLOCKS + 1, LANES), f32),
            pltpu.VMEM((bands + BLOCKS, LANES), f32),
            pltpu.VMEM((n_col - 1, bands + BLOCKS, LANES), f32),
            pltpu.SemaphoreType.DMA,
            pltpu.SemaphoreType.DMA,
            pltpu.SemaphoreType.DMA,
            pltpu.SemaphoreType.DMA((n_row - 1,)),
            pltpu.SemaphoreType.DMA,
            pltpu.SemaphoreType.DMA((n_col - 1,)),
            pltpu.SemaphoreType.DMA((bands, blocks)),
            pltpu.SemaphoreType.DMA((len(consts),)),
        ],
        compiler_params=pltpu.CompilerParams(
            collective_id=0, has_side_effects=True, vmem_limit_bytes=59 << 20),
        name="chain",
    )(x, *[jnp.asarray(t) for t in consts])

    return pl.pallas_call(
        finish_kernel,
        out_shape=jax.ShapeDtypeStruct(x.shape, f32),
        in_specs=[vmem, vmem],
        out_specs=hbm,
        scratch_shapes=[
            pltpu.VMEM((height, width), f32),
            pltpu.SemaphoreType.DMA((bands,)),
        ],
        compiler_params=pltpu.CompilerParams(vmem_limit_bytes=16 << 20),
        name="finish",
    )(u, offsets)


def solution(mesh):
    n_row, n_col = mesh.shape["row"], mesh.shape["col"]
    return jax.shard_map(
        functools.partial(per_device, n_row, n_col), mesh=mesh,
        in_specs=(P("row", "col"),), out_specs=P("row", "col"), check_vma=False,
    )
```
